128 devices in a mesh: seq: 64 (over z, y, x), head: 2 (over core).
Axes of the slice: x: 4, y: 4, z: 4, core: 2. Of those that a mesh axis runs over, the one named last changes fastest.
Arguments:
- acceptance_signal: bfloat16 [32768, 2048], P(('seq', 'head')), may hold values from -6 to 6
- lookup_entries: bfloat16 [32768, 2048], P(('seq', 'head')), may hold values from -6 to 6
- content_entries: bfloat16 [32768, 2048], P(('seq', 'head')), may hold values from -6 to 6
- fading_exponent_table: bfloat16 [32768, 2048], P(('seq', 'head')), may hold values from -17 to 0
- raw_control_signal: bfloat16 [32768, 2048], P(('seq', 'head')), may hold values from -6 to 6
- current_token_reward: float32 [32, 64], P('head'), may hold values from -1 to 1
- slice_scaling_factor: float32 [2048], P('head'), may hold values from 0.1 to 1.9
- result_mapping: bfloat16 [2048, 4096], P('head'), may hold values from -0.125 to 0.125
Outputs:
- time_mixed: bfloat16 [32768, 4096], P(('seq', 'head'))
The draws below stay inside these ranges and needn't reach their ends.
All inputs are finite; a program needn't handle non-finite values.
Results may differ from the reference program's by a relative error of at most 0.009.
Values may be sent and summed in bfloat16 or wider, within the bound.
No kernel may reach another device: no remote copies, remote signals or barrier semaphores. Data moves between devices by JAX's collectives and lax.ppermute only.
A program may use at most 192 MiB of HBM per device.

```python
import math
import jax
import jax.numpy as jnp
from jax import lax

D = 4096
ATTENTION_SLICES = 32
SLICE_BREADTH = 64
BLOCK = 128
TOK_SEQ = 512
TOKEN_SPAN = 32768


def draw_fading_exponent_table(key, part):
    hidden_breadth = ATTENTION_SLICES * SLICE_BREADTH
    lookup_lines = jax.random.split(jax.random.fold_in(key, 7), 7)
    share = 0.5
    fast_heads = jax.random.uniform(lookup_lines[0], (ATTENTION_SLICES,)) < share
    fast_rate = jnp.exp(jax.random.uniform(lookup_lines[1], (ATTENTION_SLICES, SLICE_BREADTH), jnp.float32, math.log(1.0 / 50.0), math.log(1.0 / 30.0)))
    slow_rate = jnp.exp(jax.random.uniform(lookup_lines[2], (ATTENTION_SLICES, SLICE_BREADTH), jnp.float32, math.log(1.0 / (8.0 * TOK_SEQ)), math.log(1.0 / TOK_SEQ)))
    base = jnp.where(fast_heads[:, None], fast_rate, slow_rate).reshape(hidden_breadth)
    token_factor = jnp.exp(jax.random.uniform(lookup_lines[3], (TOKEN_SPAN, hidden_breadth), jnp.float32, -math.log(2.0), math.log(2.0)))
    groups = TOKEN_SPAN // TOK_SEQ
    group_factor = jnp.exp(jax.random.uniform(lookup_lines[4], (groups, 1, hidden_breadth), jnp.float32, -math.log(2.0), math.log(2.0)))
    fading_quickness = (token_factor.reshape(groups, TOK_SEQ, hidden_breadth) * group_factor).reshape(TOKEN_SPAN, hidden_breadth) * base[None]
    spike_location = jax.random.randint(lookup_lines[5], (3,), 0, TOKEN_SPAN)
    spike_portion = jax.random.uniform(lookup_lines[6], (3, hidden_breadth), jnp.float32, 0.2, 0.5)
    spike_quickness = -jnp.log(1.0 - spike_portion)
    indicator_selector = (jnp.arange(TOKEN_SPAN)[:, None] == spike_location[None, :]).astype(jnp.float32)
    fading_quickness = fading_quickness + jnp.dot(indicator_selector, spike_quickness)
    return jnp.log(fading_quickness).astype(jnp.bfloat16)


def level_of(key, shape, cuts, least, high):
    level, own = 1.0, jax.random.fold_in(key, 6)
    for axis_at, shards_of in cuts:
        heights = jnp.exp(jax.random.uniform(jax.random.fold_in(own, axis_at), (shards_of,), jnp.float32, least / len(cuts), high / len(cuts)))
        level = level * jnp.repeat(heights, shape[axis_at] // shards_of).reshape([-1 if axis == axis_at else 1 for axis in range(len(shape))])
    return level


def normal_values(own_key, dims, width, most, cuts=(), dtype=jnp.bfloat16):
    loudness = level_of(own_key, dims, cuts, -0.22, 0.18) if cuts else 1.0
    drawn = jax.random.normal(own_key, dims, jnp.float32) * width * loudness
    return jnp.minimum(jnp.maximum(drawn, -most), most).astype(dtype)


def setup_inputs(seed: int = 0) -> dict:
    key_of = jax.random.split(jax.random.key(seed), 9)
    acceptance_signal = normal_values(key_of[0], (TOKEN_SPAN, ATTENTION_SLICES * SLICE_BREADTH), 1.0, 6.0, ((0, 128),))
    lookup_entries = normal_values(key_of[1], (TOKEN_SPAN, ATTENTION_SLICES * SLICE_BREADTH), 1.0, 6.0, ((0, 128),))
    content_entries = normal_values(key_of[2], (TOKEN_SPAN, ATTENTION_SLICES * SLICE_BREADTH), 1.0, 6.0, ((0, 128),))
    fading_exponent_table = draw_fading_exponent_table(jax.random.fold_in(key_of[8], 71), 0)
    raw_control_signal = normal_values(key_of[4], (TOKEN_SPAN, ATTENTION_SLICES * SLICE_BREADTH), 1.0, 6.0, ((0, 128),))
    current_token_reward = jnp.clip(jax.random.uniform(key_of[5], (ATTENTION_SLICES, SLICE_BREADTH), jnp.float32, -1.0, 1.0) * level_of(key_of[5], (ATTENTION_SLICES, SLICE_BREADTH), ((0, 2),), -0.4, 0.0), -1.0, 1.0)
    slice_scaling_factor = jnp.clip(1.0 + 0.18 * jax.random.normal(key_of[6], (ATTENTION_SLICES * SLICE_BREADTH,), jnp.float32), 0.1, 1.9)
    result_mapping = normal_values(key_of[7], (ATTENTION_SLICES * SLICE_BREADTH, D), (ATTENTION_SLICES * SLICE_BREADTH) ** -0.5, 0.125, ((0, 2),))
    return {"acceptance_signal": acceptance_signal, "lookup_entries": lookup_entries, "content_entries": content_entries, "fading_exponent_table": fading_exponent_table, "raw_control_signal": raw_control_signal, "current_token_reward": current_token_reward, "slice_scaling_factor": slice_scaling_factor, "result_mapping": result_mapping}


EPS = 1e-05

def reference(acceptance_signal, lookup_entries, content_entries, fading_exponent_table, raw_control_signal, current_token_reward, slice_scaling_factor, result_mapping):
    length = acceptance_signal.shape[0]
    blocks = length // BLOCK
    high = lax.Precision.HIGHEST
    hidden_breadth = ATTENTION_SLICES * SLICE_BREADTH
    positions = jnp.arange(BLOCK)
    strict = (positions[:, None] > positions[None, :]).astype(jnp.float32)
    gain = slice_scaling_factor.reshape(ATTENTION_SLICES, SLICE_BREADTH)

    def block_step(state, inputs):
        rec_in, key_in, val_in, logit_in, gate_in = inputs
        acceptance_single_real = rec_in.astype(jnp.float32)
        lookup_single_real = key_in.astype(jnp.float32)
        content_single_real = val_in.astype(jnp.float32)
        log_decay = -jnp.exp(logit_in.astype(jnp.float32))
        cum_incl = jnp.cumsum(log_decay, axis=0)
        cum_excl = cum_incl - log_decay
        total = cum_incl[-1]
        rec_scaled = acceptance_single_real * jnp.exp(cum_excl)
        key_scaled = lookup_single_real * jnp.exp(-cum_incl)
        key_ending = lookup_single_real * jnp.exp(total[None] - cum_incl)
        scores = jnp.einsum('thi,shi->hts', rec_scaled, key_scaled, precision=high) * strict[None]
        within = jnp.einsum('hts,shj->thj', scores, content_single_real, precision=high)
        diagonal_contribution = lax.optimization_barrier(jnp.sum(acceptance_single_real * current_token_reward[None] * lookup_single_real, axis=-1, keepdims=True)) * content_single_real
        across = jnp.einsum('thi,hij->thj', rec_scaled, state, precision=high)
        output = within + diagonal_contribution + across
        new_state = jnp.exp(total)[..., None] * state + jnp.einsum('shi,shj->hij', key_ending, content_single_real, precision=high)
        mean = lax.optimization_barrier(jnp.mean(output, axis=-1, keepdims=True))
        centred = output - mean
        var = lax.optimization_barrier(jnp.mean(centred * centred, axis=-1, keepdims=True))
        normed = centred / jnp.sqrt(var + EPS) * gain[None]
        gate_f = gate_in.astype(jnp.float32)
        gated = (normed.reshape(BLOCK, hidden_breadth) * jax.nn.silu(gate_f)).astype(jnp.bfloat16)
        return (new_state, gated)
    shape4 = (blocks, BLOCK, ATTENTION_SLICES, SLICE_BREADTH)
    inputs = (acceptance_signal.reshape(shape4), lookup_entries.reshape(shape4), content_entries.reshape(shape4), fading_exponent_table.reshape(shape4), raw_control_signal.reshape(blocks, BLOCK, hidden_breadth))
    start = jnp.zeros((ATTENTION_SLICES, SLICE_BREADTH, SLICE_BREADTH), jnp.float32)
    final_state, gated = lax.scan(block_step, start, inputs)
    gated = gated.reshape(length, hidden_breadth)
    return jnp.dot(gated, result_mapping, preferred_element_type=jnp.float32).astype(jnp.bfloat16)
```

```python
import functools

import jax
import jax.numpy as jnp
from jax import lax
from jax.experimental import pallas as pl
from jax.experimental.pallas import tpu as pltpu
from jax.sharding import Mesh
from jax.sharding import PartitionSpec as P

BLOCK = 128
HALF = 64
PAIR = 128
WIDE = 256
SEQ_HEAD = ("seq_0", "seq_1", "seq_2", "head")
EPS = 1e-05
BF = jnp.bfloat16
F32 = jnp.float32


def mm(a, b):
    return lax.dot_general(a, b, (((1,), (0,)), ((), ())), preferred_element_type=F32)


def mm_nt(a, b):
    return lax.dot_general(a, b, (((1,), (1,)), ((), ())), preferred_element_type=F32)


def mm_tn(a, b):
    return lax.dot_general(a, b, (((0,), (0,)), ((), ())), preferred_element_type=F32)


def grid2(rows, cols):
    return (
        lax.broadcasted_iota(jnp.int32, (rows, cols), 0),
        lax.broadcasted_iota(jnp.int32, (rows, cols), 1),
    )


def two_parts(x):
    hi = x.astype(BF)
    return hi, (x - hi.astype(F32)).astype(BF)


def head_ones(scale):
    row, col = grid2(WIDE, WIDE)
    return jnp.where(row // HALF == col // HALF, scale, 0.0).astype(BF)


def state_kernel(k_ref, v_ref, w_ref, msg_ref):
    tokens = k_ref.shape[0]
    log_decay = -jnp.exp(w_ref[...].astype(F32))
    hi, lo = two_parts(log_decay)
    row, col = grid2(tokens, tokens)
    later = jnp.where(col > row, 1.0, 0.0).astype(BF)
    after = mm(later, hi) + mm(later, lo)
    key_end = (k_ref[...].astype(F32) * jnp.exp(after)).astype(BF)
    total = after[0:1] + log_decay[0:1]
    state = mm_tn(v_ref[...], key_end)
    tot_hi, tot_lo = two_parts(total)
    tot_hi, tot_lo = tot_hi.astype(F32), tot_lo.astype(F32)
    first = lax.broadcasted_iota(jnp.int32, (HALF, PAIR), 1) < HALF
    sub = lax.broadcasted_iota(jnp.int32, (8, PAIR), 0)
    for p in range(WIDE // PAIR):
        at = p * PAIR
        both = jnp.where(
            first, state[at : at + HALF, at : at + PAIR], state[at + HALF : at + PAIR, at : at + PAIR]
        )
        logs = jnp.where(
            sub == 0,
            jnp.broadcast_to(tot_hi[:, at : at + PAIR], (8, PAIR)),
            jnp.where(sub == 1, jnp.broadcast_to(tot_lo[:, at : at + PAIR], (8, PAIR)), 0.0),
        )
        rows = jnp.concatenate(
            [both.reshape(8, 8, PAIR), jnp.broadcast_to(logs[None], (8, 8, PAIR))], axis=1
        )
        msg_ref[p * 8 : p * 8 + 8] = rows.astype(BF)


def local_kernel(r_ref, k_ref, v_ref, w_ref, u_ref, out_ref, rin_ref):
    tokens = r_ref.shape[0]
    log_decay = -jnp.exp(w_ref[...].astype(F32))
    hi, lo = two_parts(log_decay)
    row, col = grid2(tokens, tokens)
    upto = jnp.where(col <= row, 1.0, 0.0).astype(BF)
    cum = mm(upto, hi) + mm(upto, lo)
    before = cum - log_decay
    r = r_ref[...].astype(F32)
    k = k_ref[...].astype(F32)
    v = v_ref[...]
    mid0, end0, mid1 = cum[63:64], cum[127:128], cum[191:192]
    r0 = r[:BLOCK] * jnp.exp(before[:BLOCK] - mid0)
    k0 = k[:BLOCK] * jnp.exp(mid0 - cum[:BLOCK])
    r1 = r[BLOCK:] * jnp.exp(before[BLOCK:] - mid1)
    k1 = k[BLOCK:] * jnp.exp(mid1 - cum[BLOCK:])
    r1c = r1 * jnp.exp(mid1 - end0)
    k0c = k0 * jnp.exp(end0 - mid0)
    rin_ref[:BLOCK] = (r0 * jnp.exp(mid0)).astype(BF)
    rin_ref[BLOCK:] = (r1c * jnp.exp(end0)).astype(BF)
    own = mm((r * u_ref[...] * k).astype(BF), head_ones(1.0)) * v.astype(F32)
    r0, k0, r1, k1, r1c, k0c = (x.astype(BF) for x in (r0, k0, r1, k1, r1c, k0c))
    lane = lax.broadcasted_iota(jnp.int32, (BLOCK, PAIR), 1)
    first = lane < HALF
    zero = jnp.zeros((BLOCK, PAIR), BF)
    row, col = grid2(BLOCK, BLOCK)
    strict = row > col

    def stacked(x):
        return jnp.concatenate([jnp.where(first, x, zero), jnp.where(first, zero, x)], axis=0)

    def side(scores, masked):
        a, b = scores[:BLOCK], scores[BLOCK:]
        if masked:
            a, b = jnp.where(strict, a, 0.0), jnp.where(strict, b, 0.0)
        return jnp.concatenate([a, b], axis=1).astype(BF)

    for p in range(WIDE // PAIR):
        s = slice(p * PAIR, (p + 1) * PAIR)
        s00 = side(mm_nt(stacked(r0[:, s]), k0[:, s]), True)
        s10 = side(mm_nt(stacked(r1c[:, s]), k0c[:, s]), False)
        s11 = side(mm_nt(stacked(r1[:, s]), k1[:, s]), True)
        v0, v1 = stacked(v[:BLOCK, s]), stacked(v[BLOCK:, s])
        out_ref[:BLOCK, s] = mm(s00, v0) + own[:BLOCK, s]
        out_ref[BLOCK:, s] = mm(s10, v0) + mm(s11, v1) + own[BLOCK:, s]


def scan_kernel(msg_ref, out_ref):
    groups = msg_ref.shape[0]
    state = jnp.zeros((8, PAIR), F32)
    for g in range(groups):
        block = msg_ref[g].astype(F32)
        out_ref[g] = state.astype(BF)
        decay = jnp.exp(block[8:9] + block[9:10])
        state = state * decay + block[:8]


def finish_kernel(c_ref, out_ref, rin_ref, s_ref, g_ref, gain_ref, w1_ref, w2_ref, y_ref, gated):
    step = pl.program_id(0)
    chunks = gated.shape[0]

    @pl.when(step < chunks)
    def _():
        lane = lax.broadcasted_iota(jnp.int32, (HALF, PAIR), 1)
        first = lane < HALF
        zero = jnp.zeros((HALF, PAIR), BF)
        a, b = s_ref[0], s_ref[1]
        entering = jnp.concatenate(
            [
                jnp.concatenate([jnp.where(first, a, zero), zero], axis=1),
                jnp.concatenate([jnp.where(first, zero, a), zero], axis=1),
                jnp.concatenate([zero, jnp.where(first, b, zero)], axis=1),
                jnp.concatenate([zero, jnp.where(first, zero, b)], axis=1),
            ],
            axis=0,
        )
        wkv = out_ref[...] + mm_nt(rin_ref[...], entering)
        share = head_ones(1.0 / HALF)
        hi, lo = two_parts(wkv)
        centred = wkv - (mm(hi, share) + mm(lo, share))
        var = mm((centred * centred).astype(BF), share)
        gate = g_ref[...].astype(F32)
        silu = 0.5 * gate * (1.0 + jnp.tanh(0.5 * gate))
        gated[step] = (centred * lax.rsqrt(var + EPS) * gain_ref[...] * silu).astype(BF)

    @pl.when(step >= chunks)
    def _():
        half = chunks // 2
        acc = jnp.zeros(y_ref.shape, F32)
        for j in range(half):
            acc += mm(gated[j], w1_ref[j * WIDE : (j + 1) * WIDE])
        for j in range(half):
            acc += mm(gated[half + j], w2_ref[j * WIDE : (j + 1) * WIDE])
        y_ref[...] = acc.astype(BF)


def params(*semantics):
    return pltpu.CompilerParams(dimension_semantics=semantics, vmem_limit_bytes=48 << 20)


def shards(r, k, v, w, g, bonus, gain, weight):
    tokens, width = r.shape
    chunks = width // WIDE
    groups = lax.axis_size(SEQ_HEAD)
    pairs = width // PAIR
    core = lax.axis_index("head")
    swap = [(0, 1), (1, 0)]
    other_weight = lax.ppermute(weight, "head", swap)
    small = jnp.stack([bonus.reshape(-1), gain])
    other_small = lax.ppermute(small, "head", swap)
    low = jnp.where(core == 0, small, other_small)
    high = jnp.where(core == 0, other_small, small)
    small = jnp.concatenate([low, high], axis=1)
    bonus, gain = small[0:1], small[1:2]

    block = pl.BlockSpec((tokens, WIDE), lambda i: (0, i))
    per = groups // chunks
    msg = pl.pallas_call(
        state_kernel,
        grid=(chunks,),
        in_specs=[block] * 3,
        out_specs=pl.BlockSpec((per, 16, PAIR), lambda i: (i, 0, 0)),
        out_shape=jax.ShapeDtypeStruct((groups, 16, PAIR), BF),
        compiler_params=params("arbitrary"),
        cost_estimate=pl.CostEstimate(flops=4 << 30, bytes_accessed=4 << 20, transcendentals=1 << 20),
        name="state",
    )(k, v, w)
    msg = lax.all_to_all(msg, SEQ_HEAD, split_axis=0, concat_axis=0, tiled=True)

    def local(first, count):
        blk = pl.BlockSpec((tokens, WIDE), lambda i: (0, i + first))
        out_blk = pl.BlockSpec((tokens, WIDE), lambda i: (0, i))
        return pl.pallas_call(
            local_kernel,
            grid=(count,),
            in_specs=[blk] * 4 + [pl.BlockSpec((1, WIDE), lambda i: (0, i + first))],
            out_specs=[out_blk, out_blk],
            out_shape=[
                jax.ShapeDtypeStruct((tokens, count * WIDE), F32),
                jax.ShapeDtypeStruct((tokens, count * WIDE), BF),
            ],
            compiler_params=params("arbitrary"),
            cost_estimate=pl.CostEstimate(
                flops=8 << 30, bytes_accessed=10 << 20, transcendentals=4 << 20
            ),
            name="local",
        )(r, k, v, w, bonus)

    out, rin = local(0, chunks)
    entering = pl.pallas_call(
        scan_kernel,
        out_shape=jax.ShapeDtypeStruct((groups, 8, PAIR), BF),
        compiler_params=params(),
        name="scan",
    )(msg)
    entering = lax.all_to_all(entering, SEQ_HEAD, split_axis=0, concat_axis=0, tiled=True)
    entering = entering.reshape(pairs, HALF, PAIR)

    cols = weight.shape[1]
    tile = 512
    tiles = cols // tile

    def chan(i, c):
        return lax.rem(jnp.minimum(i, chunks - 1) + c[0] * (chunks // 2), chunks)

    chan_block = pl.BlockSpec((tokens, WIDE), lambda i, c: (0, chan(i, c)))
    w_block = pl.BlockSpec((width // 2, tile), lambda i, c: (0, jnp.maximum(i - chunks, 0)))
    return pl.pallas_call(
        finish_kernel,
        grid_spec=pltpu.PrefetchScalarGridSpec(
            num_scalar_prefetch=1,
            grid=(chunks + tiles,),
            in_specs=[
                chan_block,
                chan_block,
                pl.BlockSpec((2, HALF, PAIR), lambda i, c: (chan(i, c), 0, 0)),
                chan_block,
                pl.BlockSpec((1, WIDE), lambda i, c: (0, chan(i, c))),
                w_block,
                w_block,
            ],
            out_specs=pl.BlockSpec((tokens, tile), lambda i, c: (0, jnp.maximum(i - chunks, 0))),
            scratch_shapes=[pltpu.VMEM((chunks, tokens, WIDE), BF)],
        ),
        out_shape=jax.ShapeDtypeStruct((tokens, cols), BF),
        compiler_params=params("arbitrary"),
        name="finish",
    )(core.reshape(1).astype(jnp.int32), out, rin, entering, g, gain, weight, other_weight)


def solution(mesh):
    torus = Mesh(mesh.devices.reshape(4, 4, 4, mesh.shape["head"]), SEQ_HEAD)
    in_specs = (P(SEQ_HEAD, None),) * 5 + (P("head", None), P("head"), P("head", None))
    return jax.shard_map(
        shards, mesh=torus, in_specs=in_specs, out_specs=P(SEQ_HEAD, None), check_vma=False
    )
```

```python
import functools

import jax
import jax.numpy as jnp
from jax import lax
from jax.experimental import pallas as pl
from jax.experimental.pallas import tpu as pltpu
from jax.sharding import Mesh
from jax.sharding import PartitionSpec as P

BLOCK = 128
HALF = 64
PAIR = 128
WIDE = 256
SEQ_HEAD = ("seq_0", "seq_1", "seq_2", "head")
EPS = 1e-05
BF = jnp.bfloat16
F32 = jnp.float32


def mm(a, b):
    return lax.dot_general(a, b, (((1,), (0,)), ((), ())), preferred_element_type=F32)


def mm_nt(a, b):
    return lax.dot_general(a, b, (((1,), (1,)), ((), ())), preferred_element_type=F32)


def mm_tn(a, b):
    return lax.dot_general(a, b, (((0,), (0,)), ((), ())), preferred_element_type=F32)


def grid2(rows, cols):
    return (
        lax.broadcasted_iota(jnp.int32, (rows, cols), 0),
        lax.broadcasted_iota(jnp.int32, (rows, cols), 1),
    )


def two_parts(x):
    hi = x.astype(BF)
    return hi, (x - hi.astype(F32)).astype(BF)


def head_ones(scale):
    row, col = grid2(WIDE, WIDE)
    return jnp.where(row // HALF == col // HALF, scale, 0.0).astype(BF)


def centred(v):
    return (v.astype(F32) - mm(v, head_ones(1.0 / HALF))).astype(BF)


def state_kernel(k_hbm, v_hbm, w_hbm, msg_hbm, k_buf, v_buf, w_buf, msg_buf, in_sems, out_sems):
    tokens, width = k_buf.shape
    chunks = in_sems.shape[1]
    wide = width // chunks
    per = msg_buf.shape[0] // chunks
    loads = [
        [
            pltpu.make_async_copy(
                src.at[:, pl.ds(i * wide, wide)], dst.at[:, pl.ds(i * wide, wide)], in_sems.at[j, i]
            )
            for j, (src, dst) in enumerate(((w_hbm, w_buf), (k_hbm, k_buf), (v_hbm, v_buf)))
        ]
        for i in range(chunks)
    ]
    stores = [
        pltpu.make_async_copy(
            msg_buf.at[pl.ds(i * per, per)], msg_hbm.at[pl.ds(i * per, per)], out_sems.at[i]
        )
        for i in range(chunks)
    ]
    for chunk in loads:
        for one in chunk:
            one.start()
    row, col = grid2(tokens, tokens)
    later = jnp.where(col > row, 1.0, 0.0).astype(BF)
    first = lax.broadcasted_iota(jnp.int32, (HALF, PAIR), 1) < HALF
    for i in range(chunks):
        for one in loads[i]:
            one.wait()
        for part in range(i * wide // WIDE, (i + 1) * wide // WIDE):
            s = slice(part * WIDE, (part + 1) * WIDE)
            log_decay = -jnp.exp(w_buf[:, s].astype(F32))
            hi, lo = two_parts(log_decay)
            after = mm(later, hi) + mm(later, lo)
            key_end = (k_buf[:, s].astype(F32) * jnp.exp(after)).astype(BF)
            total = after[0:1] + log_decay[0:1]
            state = mm_tn(v_buf[:, s], key_end)
            tot_hi, tot_lo = two_parts(total)
            logs = jnp.concatenate([tot_hi, tot_lo], axis=0)
            for p in range(WIDE // PAIR):
                at = p * PAIR
                both = jnp.where(
                    first,
                    state[at : at + HALF, at : at + PAIR],
                    state[at + HALF : at + PAIR, at : at + PAIR],
                )
                both = (both - jnp.mean(both, axis=0, keepdims=True)).astype(BF)
                base = (part * (WIDE // PAIR) + p) * 8
                msg_buf[base : base + 8, 0:4] = both.reshape(8, 4, 2, PAIR)
                msg_buf[base : base + 8, 4] = jnp.broadcast_to(
                    logs[None, :, at : at + PAIR], (8, 2, PAIR)
                )
        stores[i].start()
    for one in stores:
        one.wait()


def local_kernel(
    r_ref, k_ref, v_ref, w_ref, g_ref, u_ref, gain_ref, out_ref, rin_ref, sg_ref
):
    tokens = r_ref.shape[0]
    row, col = grid2(tokens, tokens)
    upto = jnp.where(col <= row, 1.0, 0.0).astype(BF)
    lane = lax.broadcasted_iota(jnp.int32, (BLOCK, PAIR), 1)
    first = lane < HALF
    zero = jnp.zeros((BLOCK, PAIR), BF)
    row, col = grid2(BLOCK, BLOCK)
    strict = row > col

    def stacked(x):
        return jnp.concatenate([jnp.where(first, x, zero), jnp.where(first, zero, x)], axis=0)

    def side(scores, masked):
        a, b = scores[:BLOCK], scores[BLOCK:]
        if masked:
            a, b = jnp.where(strict, a, 0.0), jnp.where(strict, b, 0.0)
        return jnp.concatenate([a, b], axis=1).astype(BF)

    for part in range(r_ref.shape[1] // WIDE):
        at = part * WIDE
        c = slice(at, at + WIDE)
        gate = g_ref[:, c].astype(F32)
        sg_ref[:, c] = (0.5 * gate * (1.0 + jnp.tanh(0.5 * gate)) * gain_ref[:, c]).astype(BF)
        log_decay = -jnp.exp(w_ref[:, c].astype(F32))
        hi, lo = two_parts(log_decay)
        cum = mm(upto, hi) + mm(upto, lo)
        before = cum - log_decay
        r = r_ref[:, c].astype(F32)
        k = k_ref[:, c].astype(F32)
        v = centred(v_ref[:, c])
        mid0, end0, mid1 = cum[63:64], cum[127:128], cum[191:192]
        r0 = r[:BLOCK] * jnp.exp(before[:BLOCK] - mid0)
        k0 = k[:BLOCK] * jnp.exp(mid0 - cum[:BLOCK])
        r1 = r[BLOCK:] * jnp.exp(before[BLOCK:] - mid1)
        k1 = k[BLOCK:] * jnp.exp(mid1 - cum[BLOCK:])
        r1c = r1 * jnp.exp(mid1 - end0)
        k0c = k0 * jnp.exp(end0 - mid0)
        rin_ref[:BLOCK, c] = (r0 * jnp.exp(mid0)).astype(BF)
        rin_ref[BLOCK:, c] = (r1c * jnp.exp(end0)).astype(BF)
        own = mm((r * u_ref[:, c] * k).astype(BF), head_ones(1.0)) * v.astype(F32)
        r0, k0, r1, k1, r1c, k0c = (x.astype(BF) for x in (r0, k0, r1, k1, r1c, k0c))
        for p in range(WIDE // PAIR):
            s = slice(p * PAIR, (p + 1) * PAIR)
            o = slice(at + p * PAIR, at + (p + 1) * PAIR)
            s00 = side(mm_nt(stacked(r0[:, s]), k0[:, s]), True)
            s10 = side(mm_nt(stacked(r1c[:, s]), k0c[:, s]), False)
            s11 = side(mm_nt(stacked(r1[:, s]), k1[:, s]), True)
            v0, v1 = stacked(v[:BLOCK, s]), stacked(v[BLOCK:, s])
            out_ref[:BLOCK, o] = mm(s00, v0) + own[:BLOCK, s]
            out_ref[BLOCK:, o] = mm(s10, v0) + mm(s11, v1) + own[BLOCK:, s]


def scan_kernel(msg_ref, after_ref, out_ref):
    groups = msg_ref.shape[0]
    state = jnp.zeros((8, PAIR), F32)
    for g in range(groups):
        logs = msg_ref[g, 4].astype(F32)
        out_ref[g] = state.astype(BF)
        decay = jnp.exp(logs[0:1] + logs[1:2])
        state = state * decay + msg_ref[g, 0:4].reshape(8, PAIR).astype(F32)


def finish_kernel(
    c_ref,
    s_hbm,
    out_hbm,
    rin_hbm,
    sg_hbm,
    w1_hbm,
    w2_hbm,
    y_hbm,
    s_ref,
    out_buf,
    rin_buf,
    sg_buf,
    w_buf,
    gated,
    y_buf,
    s_sem,
    in_sems,
    w_sems,
    y_sems,
):
    chunks = in_sems.shape[1]
    tiles = y_sems.shape[0]
    wide = out_buf.shape[1] // chunks
    tile = y_buf.shape[1] // tiles
    half = out_buf.shape[1] // 2
    loads = [
        [
            pltpu.make_async_copy(
                src.at[:, pl.ds(i * wide, wide)], dst.at[:, pl.ds(i * wide, wide)], in_sems.at[j, i]
            )
            for j, (src, dst) in enumerate(((out_hbm, out_buf), (rin_hbm, rin_buf), (sg_hbm, sg_buf)))
        ]
        for i in range(chunks)
    ]

    def cols(t):
        return pl.ds(pl.multiple_of(t * tile, tile), tile)

    def fetch(j, t):
        src = (w1_hbm, w2_hbm)[j]
        return pltpu.make_async_copy(src.at[:, cols(t)], w_buf.at[j, :, cols(t)], w_sems.at[j, t])

    def store(t):
        return pltpu.make_async_copy(y_buf.at[:, cols(t)], y_hbm.at[:, cols(t)], y_sems.at[t])

    entering_load = pltpu.make_async_copy(s_hbm, s_ref, s_sem)
    entering_load.start()
    for chunk in loads:
        for one in chunk:
            one.start()
    entering_load.wait()
    first = lax.broadcasted_iota(jnp.int32, (HALF, PAIR), 1) < HALF
    zero = jnp.zeros((HALF, PAIR), BF)
    share = head_ones(1.0 / HALF)
    for i in range(chunks):
        for one in loads[i]:
            one.wait()
        fetch(0, i).start()
        fetch(1, i).start()
        for part in range(i * wide // WIDE, (i + 1) * wide // WIDE):
            c = slice(part * WIDE, (part + 1) * WIDE)
            a, b = s_ref[2 * part], s_ref[2 * part + 1]
            entering = jnp.concatenate(
                [
                    jnp.concatenate([jnp.where(first, a, zero), zero], axis=1),
                    jnp.concatenate([jnp.where(first, zero, a), zero], axis=1),
                    jnp.concatenate([zero, jnp.where(first, b, zero)], axis=1),
                    jnp.concatenate([zero, jnp.where(first, zero, b)], axis=1),
                ],
                axis=0,
            )
            wkv = out_buf[:, c] + mm_nt(rin_buf[:, c], entering)
            var = mm((wkv * wkv).astype(BF), share)
            to = part * WIDE % half
            gated[part * WIDE // half, :, to : to + WIDE] = (
                wkv * lax.rsqrt(var + EPS) * sg_buf[:, c].astype(F32)
            ).astype(BF)

    mine = c_ref[0]

    def project(t, carry):
        fetch(0, t).wait()
        fetch(1, t).wait()

        @pl.when(t + chunks < tiles)
        def _():
            fetch(0, t + chunks).start()
            fetch(1, t + chunks).start()

        y = mm(gated[mine], w_buf[0, :, cols(t)]) + mm(gated[1 - mine], w_buf[1, :, cols(t)])
        y_buf[:, cols(t)] = y.astype(BF)
        store(t).start()
        return carry

    lax.fori_loop(0, tiles, project, 0)
    for t in range(tiles):
        store(t).wait()


def params(*semantics, limit=66_000_000):
    return pltpu.CompilerParams(dimension_semantics=semantics, vmem_limit_bytes=limit)


def call_state(k, v, w, groups):
    chunks = 4
    any_block = pl.BlockSpec(memory_space=pl.ANY)
    shape = (groups, 5, 2, PAIR)
    return pl.pallas_call(
        state_kernel,
        in_specs=[any_block] * 3,
        out_specs=any_block,
        out_shape=jax.ShapeDtypeStruct(shape, BF),
        scratch_shapes=[pltpu.VMEM(k.shape, BF)] * 3
        + [
            pltpu.VMEM(shape, BF),
            pltpu.SemaphoreType.DMA((3, chunks)),
            pltpu.SemaphoreType.DMA((chunks,)),
        ],
        compiler_params=params(),
        cost_estimate=pl.CostEstimate(flops=4 << 30, bytes_accessed=4 << 20, transcendentals=1 << 20),
        name="state",
    )(k, v, w)


def call_local(r, k, v, w, g, bonus, gain, start, count):
    tokens = r.shape[0]
    wide = 2 * WIDE
    blk = pl.BlockSpec((tokens, wide), lambda i: (0, i + start))
    row = pl.BlockSpec((1, wide), lambda i: (0, i + start))
    out_blk = pl.BlockSpec((tokens, wide), lambda i: (0, i))
    return pl.pallas_call(
        local_kernel,
        grid=(count,),
        in_specs=[blk] * 5 + [row] * 2,
        out_specs=[out_blk] * 3,
        out_shape=[jax.ShapeDtypeStruct((tokens, count * wide), t) for t in (F32, BF, BF)],
        compiler_params=params("arbitrary"),
        cost_estimate=pl.CostEstimate(flops=4 << 30, bytes_accessed=10 << 20, transcendentals=4 << 20),
        name="local",
    )(r, k, v, w, g, bonus, gain)


def call_scan(msg, anchor):
    anchor = pltpu.with_memory_space_constraint(anchor, pltpu.HBM)
    return pl.pallas_call(
        scan_kernel,
        in_specs=[pl.BlockSpec(memory_space=pltpu.VMEM), pl.BlockSpec(memory_space=pl.ANY)],
        out_shape=jax.ShapeDtypeStruct((msg.shape[0], 8, PAIR), BF),
        compiler_params=params(limit=8 << 20),
        name="scan",
    )(msg, anchor)


def call_finish(core, out, rin, entering, sg, weight, other_weight):
    tokens, width = out.shape
    cols = weight.shape[1]
    chunks, tiles = 4, 8
    any_block = pl.BlockSpec(memory_space=pl.ANY)
    return pl.pallas_call(
        finish_kernel,
        in_specs=[
            pl.BlockSpec(memory_space=pltpu.SMEM),
        ]
        + [any_block] * 6,
        out_specs=any_block,
        out_shape=jax.ShapeDtypeStruct((tokens, cols), BF),
        scratch_shapes=[
            pltpu.VMEM(entering.shape, BF),
            pltpu.VMEM(out.shape, F32),
            pltpu.VMEM(out.shape, BF),
            pltpu.VMEM(out.shape, BF),
            pltpu.VMEM((2, width // 2, cols), BF),
            pltpu.VMEM((2, tokens, width // 2), BF),
            pltpu.VMEM((tokens, cols), BF),
            pltpu.SemaphoreType.DMA,
            pltpu.SemaphoreType.DMA((3, chunks)),
            pltpu.SemaphoreType.DMA((2, tiles)),
            pltpu.SemaphoreType.DMA((tiles,)),
        ],
        compiler_params=params(limit=58 << 20),
        name="finish",
    )(core.reshape(1).astype(jnp.int32), entering, out, rin, sg, weight, other_weight)


def shards(r, k, v, w, g, bonus, gain, weight):
    groups = lax.axis_size(SEQ_HEAD)
    core = lax.axis_index("head")
    r, k, v, w, g = (pltpu.with_memory_space_constraint(x, pltpu.HBM) for x in (r, k, v, w, g))
    swap = [(0, 1), (1, 0)]
    other_weight = lax.ppermute(weight, "head", swap)
    small = jnp.stack([bonus.reshape(-1), gain])
    other_small = lax.ppermute(small, "head", swap)
    low = jnp.where(core == 0, small, other_small)
    high = jnp.where(core == 0, other_small, small)
    small = jnp.concatenate([low, high], axis=1)
    bonus, gain = small[0:1], small[1:2]
    msg = call_state(k, v, w, groups)
    msg = lax.all_to_all(msg, SEQ_HEAD, split_axis=0, concat_axis=0, tiled=True)
    out, rin, sg = call_local(r, k, v, w, g, bonus, gain, 0, r.shape[1] // (2 * WIDE))
    entering = call_scan(msg, rin)
    entering = lax.all_to_all(entering, SEQ_HEAD, split_axis=0, concat_axis=0, tiled=True)
    entering = entering.reshape(-1, HALF, PAIR)
    return call_finish(core, out, rin, entering, sg, weight, other_weight)


def solution(mesh):
    torus = Mesh(mesh.devices.reshape(4, 4, 4, mesh.shape["head"]), SEQ_HEAD)
    in_specs = (P(SEQ_HEAD, None),) * 5 + (P("head", None), P("head"), P("head", None))
    return jax.shard_map(
        shards, mesh=torus, in_specs=in_specs, out_specs=P(SEQ_HEAD, None), check_vma=False
    )
```

```python
import functools

import jax
import jax.numpy as jnp
from jax import lax
from jax.experimental import pallas as pl
from jax.experimental.pallas import tpu as pltpu
from jax.sharding import Mesh
from jax.sharding import PartitionSpec as P

BLOCK = 128
HALF = 64
PAIR = 128
WIDE = 256
SEQ_HEAD = ("seq_0", "seq_1", "seq_2", "head")
EPS = 1e-05
LOG2E = 1.4426950408889634
LOG2LOG2E = 0.5287663729448977
WEIGHT_STAGES = ((0, 1), (2, 3), (4,), (5,))
WEIGHTS_AHEAD = 6
BF = jnp.bfloat16
F32 = jnp.float32


def mm(a, b):
    return lax.dot_general(a, b, (((1,), (0,)), ((), ())), preferred_element_type=F32)


def mm_nt(a, b):
    return lax.dot_general(a, b, (((1,), (1,)), ((), ())), preferred_element_type=F32)


def mm_tn(a, b):
    return lax.dot_general(a, b, (((0,), (0,)), ((), ())), preferred_element_type=F32)


def grid2(rows, cols):
    return (
        lax.broadcasted_iota(jnp.int32, (rows, cols), 0),
        lax.broadcasted_iota(jnp.int32, (rows, cols), 1),
    )


def two_parts(x):
    hi = x.astype(BF)
    return hi, (x - hi.astype(F32)).astype(BF)


def head_ones(scale):
    row, col = grid2(WIDE, WIDE)
    return jnp.where(row // HALF == col // HALF, scale, 0.0).astype(BF)


def decay_rate(w):
    return jnp.exp2(w.astype(F32) * LOG2E + LOG2LOG2E).astype(BF)


def centred(v):
    return (v.astype(F32) - mm(v, head_ones(1.0 / HALF))).astype(BF)


def state_kernel(k_hbm, v_hbm, w_hbm, msg_hbm, k_buf, v_buf, w_buf, msg_buf, in_sems, out_sems):
    tokens, width = k_buf.shape
    chunks = in_sems.shape[1]
    wide = width // chunks
    per = msg_buf.shape[0] // chunks
    loads = [
        [
            pltpu.make_async_copy(
                src.at[:, pl.ds(i * wide, wide)], dst.at[:, pl.ds(i * wide, wide)], in_sems.at[j, i]
            )
            for j, (src, dst) in enumerate(((w_hbm, w_buf), (k_hbm, k_buf), (v_hbm, v_buf)))
        ]
        for i in range(chunks)
    ]
    stores = [
        pltpu.make_async_copy(
            msg_buf.at[pl.ds(i * per, per)], msg_hbm.at[pl.ds(i * per, per)], out_sems.at[i]
        )
        for i in range(chunks)
    ]
    depth = chunks
    for chunk in loads[:depth]:
        for one in chunk:
            one.start()
    row, col = grid2(tokens, tokens)
    later = jnp.where(col > row, -1.0, 0.0).astype(BF)
    first = lax.broadcasted_iota(jnp.int32, (HALF, PAIR), 1) < HALF
    for i in range(chunks):
        for one in loads[i]:
            one.wait()
        for one in loads[i + depth] if i + depth < chunks else ():
            one.start()
        for part in range(i * wide // WIDE, (i + 1) * wide // WIDE):
            s = slice(part * WIDE, (part + 1) * WIDE)
            rate = decay_rate(w_buf[:, s])
            after = mm(later, rate)
            key_end = k_buf[:, s] * jnp.exp2(after).astype(BF)
            total = after[0:1] - rate[0:1].astype(F32)
            state = mm_tn(v_buf[:, s], key_end)
            tot_hi, tot_lo = two_parts(total)
            logs = jnp.concatenate([tot_hi, tot_lo], axis=0)
            for p in range(WIDE // PAIR):
                at = p * PAIR
                both = jnp.where(
                    first,
                    state[at : at + HALF, at : at + PAIR],
                    state[at + HALF : at + PAIR, at : at + PAIR],
                )
                both = (both - jnp.mean(both, axis=0, keepdims=True)).astype(BF)
                base = (part * (WIDE // PAIR) + p) * 8
                msg_buf[base : base + 8, 0:4] = both.reshape(8, 4, 2, PAIR)
                msg_buf[base : base + 8, 4] = jnp.broadcast_to(
                    logs[None, :, at : at + PAIR], (8, 2, PAIR)
                )
        stores[i].start()
    for one in stores:
        one.wait()


def local_kernel(
    r_ref, k_ref, v_ref, w_ref, g_ref, u_ref, gain_ref, out_ref, rin_ref, sg_ref
):
    tokens = r_ref.shape[0]
    row, col = grid2(tokens, tokens)
    upto = jnp.where(col <= row, -1.0, 0.0).astype(BF)
    prior = jnp.where(col < row, -1.0, 0.0).astype(BF)
    lane = lax.broadcasted_iota(jnp.int32, (BLOCK, PAIR), 1)
    first = lane < HALF
    zero = jnp.zeros((BLOCK, PAIR), BF)
    row, col = grid2(BLOCK, BLOCK)
    strict = row > col

    def stacked(x):
        return jnp.concatenate([jnp.where(first, x, zero), jnp.where(first, zero, x)], axis=0)

    def side(scores, masked):
        a, b = scores[:BLOCK], scores[BLOCK:]
        if masked:
            a, b = jnp.where(strict, a, 0.0), jnp.where(strict, b, 0.0)
        return jnp.concatenate([a, b], axis=1).astype(BF)

    for part in range(r_ref.shape[1] // WIDE):
        at = part * WIDE
        c = slice(at, at + WIDE)
        gate = g_ref[:, c].astype(F32)
        sg_ref[:, c] = (0.5 * gate * (1.0 + jnp.tanh(0.5 * gate)) * gain_ref[:, c]).astype(BF)
        rate = decay_rate(w_ref[:, c])
        cum = mm(upto, rate)
        before = mm(prior, rate)
        r = r_ref[:, c]
        k = k_ref[:, c]
        v = centred(v_ref[:, c])
        mid0, end0, mid1 = cum[63:64], cum[127:128], cum[191:192]
        r0 = r[:BLOCK] * jnp.exp2(before[:BLOCK] - mid0).astype(BF)
        k0 = k[:BLOCK] * jnp.exp2(mid0 - cum[:BLOCK]).astype(BF)
        r1 = r[BLOCK:] * jnp.exp2(before[BLOCK:] - mid1).astype(BF)
        k1 = k[BLOCK:] * jnp.exp2(mid1 - cum[BLOCK:]).astype(BF)
        r1c = r[BLOCK:] * jnp.exp2(before[BLOCK:] - end0).astype(BF)
        k0c = k[:BLOCK] * jnp.exp2(end0 - cum[:BLOCK]).astype(BF)
        rin_ref[:BLOCK, c] = r[:BLOCK] * jnp.exp2(before[:BLOCK]).astype(BF)
        rin_ref[BLOCK:, c] = r[BLOCK:] * jnp.exp2(before[BLOCK:]).astype(BF)
        bonus = (r.astype(F32) * u_ref[:, c] * k.astype(F32)).astype(BF)
        own = mm(bonus, head_ones(1.0)) * v.astype(F32)
        for p in range(WIDE // PAIR):
            s = slice(p * PAIR, (p + 1) * PAIR)
            o = slice(at + p * PAIR, at + (p + 1) * PAIR)
            s00 = side(mm_nt(stacked(r0[:, s]), k0[:, s]), True)
            s10 = side(mm_nt(stacked(r1c[:, s]), k0c[:, s]), False)
            s11 = side(mm_nt(stacked(r1[:, s]), k1[:, s]), True)
            v0, v1 = stacked(v[:BLOCK, s]), stacked(v[BLOCK:, s])
            out_ref[:BLOCK, o] = mm(s00, v0) + own[:BLOCK, s]
            out_ref[BLOCK:, o] = mm(s10, v0) + mm(s11, v1) + own[BLOCK:, s]


def scan_kernel(msg_ref, after_ref, out_ref):
    groups = msg_ref.shape[0]
    state = jnp.zeros((8, PAIR), F32)
    for g in range(groups):
        logs = msg_ref[g, 4].astype(F32)
        out_ref[g] = state.astype(BF)
        decay = jnp.exp2(logs[0:1] + logs[1:2])
        state = state * decay + msg_ref[g, 0:4].reshape(8, PAIR).astype(F32)


def finish_kernel(
    c_ref,
    s_ref,
    early_out,
    early_rin,
    early_sg,
    late_out,
    late_rin,
    late_sg,
    w1_hbm,
    w2_hbm,
    y_hbm,
    out_buf,
    rin_buf,
    sg_buf,
    w_buf,
    entering,
    gated,
    y_buf,
    in_sems,
    w_sems,
    y_sems,
):
    chunks = in_sems.shape[1]
    tiles = y_sems.shape[0]
    wide = out_buf.shape[1] // chunks
    tile = y_buf.shape[1] // tiles
    half = out_buf.shape[1] // 2
    split = early_out.shape[1] // wide
    loads = []
    for i in range(chunks):
        if i < split:
            at, sources = i * wide, (early_out, early_rin, early_sg)
        else:
            at, sources = (i - split) * wide, (late_out, late_rin, late_sg)
        loads.append(
            [
                pltpu.make_async_copy(
                    src.at[:, pl.ds(at, wide)], dst.at[:, pl.ds(i * wide, wide)], in_sems.at[j, i]
                )
                for j, (src, dst) in enumerate(zip(sources, (out_buf, rin_buf, sg_buf)))
            ]
        )

    def cols(t):
        return pl.ds(pl.multiple_of(t * tile, tile), tile)

    def fetch(j, t):
        src = (w1_hbm, w2_hbm)[j]
        return pltpu.make_async_copy(src.at[:, cols(t)], w_buf.at[j, :, cols(t)], w_sems.at[j, t])

    def store(t):
        return pltpu.make_async_copy(y_buf.at[:, cols(t)], y_hbm.at[:, cols(t)], y_sems.at[t])

    for chunk in loads:
        for one in chunk:
            one.start()
    first = lax.broadcasted_iota(jnp.int32, (HALF, PAIR), 1) < HALF
    zero = jnp.zeros((HALF, PAIR), BF)
    share = head_ones(1.0 / HALF)
    parts = out_buf.shape[1] // WIDE
    per = parts // chunks

    def place(part):
        to = part * WIDE % half
        return part * WIDE // half, slice(to, to + WIDE)

    for part in range(parts):
        for p in range(2):
            pair = s_ref[2 * part + p]
            lanes = slice(p * PAIR, (p + 1) * PAIR)
            rest = slice((1 - p) * PAIR, (2 - p) * PAIR)
            entering[part, p * PAIR : p * PAIR + HALF, lanes] = jnp.where(first, pair, zero)
            entering[part, p * PAIR + HALF : (p + 1) * PAIR, lanes] = jnp.where(first, zero, pair)
            entering[part, p * PAIR : (p + 1) * PAIR, rest] = jnp.zeros((PAIR, PAIR), BF)
    for i in range(chunks):
        for one in loads[i]:
            one.wait()
        for t in WEIGHT_STAGES[i]:
            fetch(0, t).start()
            fetch(1, t).start()
        for part in range(i * per, (i + 1) * per):
            c = slice(part * WIDE, (part + 1) * WIDE)
            side, to = place(part)
            wkv = out_buf[:, c] + mm_nt(rin_buf[:, c], entering[part])
            out_buf[:, c] = wkv
            gated[side, :, to] = (wkv * wkv).astype(BF)
    for part in range(parts):
        c = slice(part * WIDE, (part + 1) * WIDE)
        side, to = place(part)
        var = mm(gated[side, :, to], share)
        gated[side, :, to] = (
            out_buf[:, c] * lax.rsqrt(var + EPS) * sg_buf[:, c].astype(F32)
        ).astype(BF)

    mine = c_ref[0]

    def project(t, carry):
        fetch(0, t).wait()
        fetch(1, t).wait()

        @pl.when(t + WEIGHTS_AHEAD < tiles)
        def _():
            fetch(0, t + WEIGHTS_AHEAD).start()
            fetch(1, t + WEIGHTS_AHEAD).start()

        y = mm(gated[mine], w_buf[0, :, cols(t)]) + mm(gated[1 - mine], w_buf[1, :, cols(t)])
        y_buf[:, cols(t)] = y.astype(BF)
        store(t).start()
        return carry

    lax.fori_loop(0, tiles, project, 0)
    for t in range(tiles):
        store(t).wait()


def params(*semantics, limit=66_000_000):
    return pltpu.CompilerParams(dimension_semantics=semantics, vmem_limit_bytes=limit)


def in_hbm(x):
    return pltpu.with_memory_space_constraint(x, pltpu.HBM)


def call_state(k, v, w, groups):
    chunks = 2
    any_block = pl.BlockSpec(memory_space=pl.ANY)
    shape = (groups, 5, 2, PAIR)
    return pl.pallas_call(
        state_kernel,
        in_specs=[any_block] * 3,
        out_specs=any_block,
        out_shape=jax.ShapeDtypeStruct(shape, BF),
        scratch_shapes=[pltpu.VMEM(k.shape, BF)] * 3
        + [
            pltpu.VMEM(shape, BF),
            pltpu.SemaphoreType.DMA((3, chunks)),
            pltpu.SemaphoreType.DMA((chunks,)),
        ],
        compiler_params=params(),
        cost_estimate=pl.CostEstimate(flops=4 << 30, bytes_accessed=4 << 20, transcendentals=1 << 20),
        name="state",
    )(k, v, w)


def call_local(r, k, v, w, g, bonus, gain, start, count):
    tokens = r.shape[0]
    wide = 2 * WIDE
    blk = pl.BlockSpec((tokens, wide), lambda i: (0, i + start))
    row = pl.BlockSpec((1, wide), lambda i: (0, i + start))
    out_blk = pl.BlockSpec((tokens, wide), lambda i: (0, i))
    return pl.pallas_call(
        local_kernel,
        grid=(count,),
        in_specs=[blk] * 5 + [row] * 2,
        out_specs=[out_blk] * 3,
        out_shape=[jax.ShapeDtypeStruct((tokens, count * wide), t) for t in (F32, BF, BF)],
        compiler_params=params("arbitrary"),
        cost_estimate=pl.CostEstimate(flops=count << 32, bytes_accessed=count << 21, transcendentals=count << 20),
        name="local",
    )(r, k, v, w, g, bonus, gain)


def call_scan(msg, anchor):
    anchor = in_hbm(anchor)
    return pl.pallas_call(
        scan_kernel,
        in_specs=[pl.BlockSpec(memory_space=pltpu.VMEM), pl.BlockSpec(memory_space=pl.ANY)],
        out_shape=jax.ShapeDtypeStruct((msg.shape[0], 8, PAIR), BF),
        compiler_params=params(limit=8 << 20),
        name="scan",
    )(msg, anchor)


def call_finish(core, entering, early, late, weight, other_weight):
    tokens, width = early[0].shape[0], 2 * weight.shape[0]
    early, late = ([in_hbm(x) for x in part] for part in (early, late))
    weight, other_weight = in_hbm(weight), in_hbm(other_weight)
    cols = weight.shape[1]
    chunks, tiles = 4, 8
    any_block = pl.BlockSpec(memory_space=pl.ANY)
    return pl.pallas_call(
        finish_kernel,
        in_specs=[
            pl.BlockSpec(memory_space=pltpu.SMEM),
            pl.BlockSpec(memory_space=pltpu.VMEM),
        ]
        + [any_block] * 8,
        out_specs=any_block,
        out_shape=jax.ShapeDtypeStruct((tokens, cols), BF),
        scratch_shapes=[
            pltpu.VMEM((tokens, width), F32),
            pltpu.VMEM((tokens, width), BF),
            pltpu.VMEM((tokens, width), BF),
            pltpu.VMEM((2, width // 2, cols), BF),
            pltpu.VMEM((width // WIDE, WIDE, WIDE), BF),
            pltpu.VMEM((2, tokens, width // 2), BF),
            pltpu.VMEM((tokens, cols), BF),
            pltpu.SemaphoreType.DMA((3, chunks)),
            pltpu.SemaphoreType.DMA((2, tiles)),
            pltpu.SemaphoreType.DMA((tiles,)),
        ],
        compiler_params=params(limit=32 << 20),
        name="finish",
    )(core.reshape(1).astype(jnp.int32), entering, *early, *late, weight, other_weight)


def shards(r, k, v, w, g, bonus, gain, weight):
    groups = lax.axis_size(SEQ_HEAD)
    core = lax.axis_index("head")
    r, k, v, w, g = (in_hbm(x) for x in (r, k, v, w, g))
    swap = [(0, 1), (1, 0)]
    other_weight = lax.ppermute(weight, "head", swap)
    msg = call_state(k, v, w, groups)
    msg, bonus, gain = lax.optimization_barrier((msg, bonus, gain))
    msg = lax.all_to_all(msg, SEQ_HEAD, split_axis=0, concat_axis=0, tiled=True)
    small = jnp.stack([bonus.reshape(-1), gain])
    other_small = lax.ppermute(small, "head", swap)
    low = jnp.where(core == 0, small, other_small)
    high = jnp.where(core == 0, other_small, small)
    small = jnp.concatenate([low, high], axis=1)
    bonus, gain = small[0:1], small[1:2]
    steps = r.shape[1] // (2 * WIDE)
    first = 2
    early = call_local(r, k, v, w, g, bonus, gain, 0, first)
    entering = call_scan(msg, early[1])
    entering = lax.all_to_all(entering, SEQ_HEAD, split_axis=0, concat_axis=0, tiled=True)
    late = call_local(r, k, v, w, g, bonus, gain, first, steps - first)
    entering = entering.reshape(-1, HALF, PAIR)
    return call_finish(core, entering, early, late, weight, other_weight)


def solution(mesh):
    torus = Mesh(mesh.devices.reshape(4, 4, 4, mesh.shape["head"]), SEQ_HEAD)
    in_specs = (P(SEQ_HEAD, None),) * 5 + (P("head", None), P("head"), P("head", None))
    return jax.shard_map(
        shards, mesh=torus, in_specs=in_specs, out_specs=P(SEQ_HEAD, None), check_vma=False
    )
```

```python
import jax
import jax.numpy as jnp
from jax import lax
from jax.experimental import pallas as pl
from jax.experimental.pallas import tpu as pltpu
from jax.sharding import Mesh
from jax.sharding import PartitionSpec as P


BLOCK = 128
HALF = 64
PAIR = 128
WIDE = 256
SEQ_HEAD = ("seq_0", "seq_1", "seq_2", "head")
EPS = 1e-05
LOG2E = 1.4426950408889634
LOG2LOG2E = 0.5287663729448977
WEIGHT_STAGES = ((0, 1, 2), (3, 4), (5, 6), (7,))
TILES_AHEAD = 8
BF = jnp.bfloat16
F32 = jnp.float32


def mm(a, b):
    return lax.dot_general(a, b, (((1,), (0,)), ((), ())), preferred_element_type=F32)


def mm_nt(a, b):
    return lax.dot_general(a, b, (((1,), (1,)), ((), ())), preferred_element_type=F32)


def mm_tn(a, b):
    return lax.dot_general(a, b, (((0,), (0,)), ((), ())), preferred_element_type=F32)


def grid2(rows, cols):
    return (
        lax.broadcasted_iota(jnp.int32, (rows, cols), 0),
        lax.broadcasted_iota(jnp.int32, (rows, cols), 1),
    )


def two_parts(x):
    hi = x.astype(BF)
    return hi, (x - hi.astype(F32)).astype(BF)


def head_ones(scale):
    row, col = grid2(WIDE, WIDE)
    return jnp.where(row // HALF == col // HALF, scale, 0.0).astype(BF)


def decay_rate(w):
    return jnp.exp2(w.astype(F32) * LOG2E + LOG2LOG2E).astype(BF)


def centred(v):
    return (v.astype(F32) - mm(v, head_ones(1.0 / HALF))).astype(BF)


def state_kernel(k_hbm, v_hbm, w_hbm, msg_hbm, k_buf, v_buf, w_buf, msg_buf, in_sems, out_sems):
    tokens, width = k_buf.shape
    chunks = in_sems.shape[1]
    wide = width // chunks
    per = msg_buf.shape[0] // chunks
    loads = [
        [
            pltpu.make_async_copy(
                src.at[:, pl.ds(i * wide, wide)], dst.at[:, pl.ds(i * wide, wide)], in_sems.at[j, i]
            )
            for j, (src, dst) in enumerate(((w_hbm, w_buf), (k_hbm, k_buf), (v_hbm, v_buf)))
        ]
        for i in range(chunks)
    ]
    stores = [
        pltpu.make_async_copy(
            msg_buf.at[pl.ds(i * per, per)], msg_hbm.at[pl.ds(i * per, per)], out_sems.at[i]
        )
        for i in range(chunks)
    ]
    depth = chunks
    for chunk in loads[:depth]:
        for one in chunk:
            one.start()
    row, col = grid2(tokens, tokens)
    later = jnp.where(col > row, -1.0, 0.0).astype(BF)
    first = lax.broadcasted_iota(jnp.int32, (HALF, PAIR), 1) < HALF
    for i in range(chunks):
        for one in loads[i]:
            one.wait()
        for one in loads[i + depth] if i + depth < chunks else ():
            one.start()
        for part in range(i * wide // WIDE, (i + 1) * wide // WIDE):
            s = slice(part * WIDE, (part + 1) * WIDE)
            rate = decay_rate(w_buf[:, s])
            after = mm(later, rate)
            key_end = k_buf[:, s] * jnp.exp2(after).astype(BF)
            total = after[0:1] - rate[0:1].astype(F32)
            state = mm_tn(v_buf[:, s], key_end)
            tot_hi, tot_lo = two_parts(total)
            logs = jnp.concatenate([tot_hi, tot_lo], axis=0)
            for p in range(WIDE // PAIR):
                at = p * PAIR
                both = jnp.where(
                    first,
                    state[at : at + HALF, at : at + PAIR],
                    state[at + HALF : at + PAIR, at : at + PAIR],
                )
                both = (both - jnp.mean(both, axis=0, keepdims=True)).astype(BF)
                base = (part * (WIDE // PAIR) + p) * 8
                msg_buf[base : base + 8, 0:4] = both.reshape(8, 4, 2, PAIR)
                msg_buf[base : base + 8, 4] = jnp.broadcast_to(
                    logs[None, :, at : at + PAIR], (8, 2, PAIR)
                )
        stores[i].start()
    for one in stores:
        one.wait()


def local_kernel(
    h_ref,
    u_ref,
    gain_ref,
    r_hbm,
    k_hbm,
    v_hbm,
    w_hbm,
    g_hbm,
    out_hbm,
    rin_hbm,
    sg_hbm,
    r_ref,
    k_ref,
    v_ref,
    w_ref,
    g_ref,
    out_ref,
    rin_ref,
    sg_ref,
    in_sems,
    out_sems,
):
    tokens, half = r_ref.shape
    chunks = in_sems.shape[1]
    wide = half // chunks
    sources = (w_hbm, g_hbm, r_hbm, k_hbm, v_hbm)
    buffers = (w_ref, g_ref, r_ref, k_ref, v_ref)
    results = (out_ref, rin_ref, sg_ref)
    targets = (out_hbm, rin_hbm, sg_hbm)

    def load(i):
        at = pl.ds(pl.multiple_of(h_ref[0] * half + i * wide, wide), wide)
        to = pl.ds(i * wide, wide)
        return [
            pltpu.make_async_copy(src.at[:, at], dst.at[:, to], in_sems.at[j, i])
            for j, (src, dst) in enumerate(zip(sources, buffers))
        ]

    def store(i):
        at = pl.ds(i * wide, wide)
        return [
            pltpu.make_async_copy(src.at[:, at], dst.at[:, at], out_sems.at[j, i])
            for j, (src, dst) in enumerate(zip(results, targets))
        ]

    for i in range(chunks):
        for one in load(i):
            one.start()
    row, col = grid2(tokens, tokens)
    upto = jnp.where(col <= row, -1.0, 0.0).astype(BF)
    prior = jnp.where(col < row, -1.0, 0.0).astype(BF)
    lane = lax.broadcasted_iota(jnp.int32, (BLOCK, PAIR), 1)
    first = lane < HALF
    zero = jnp.zeros((BLOCK, PAIR), BF)
    row, col = grid2(BLOCK, BLOCK)
    strict = row > col

    def stacked(x):
        return jnp.concatenate([jnp.where(first, x, zero), jnp.where(first, zero, x)], axis=0)

    def side(scores, masked):
        a, b = scores[:BLOCK], scores[BLOCK:]
        if masked:
            a, b = jnp.where(strict, a, 0.0), jnp.where(strict, b, 0.0)
        return jnp.concatenate([a, b], axis=1).astype(BF)

    def compute(part):
        at = part * WIDE
        c = slice(at, at + WIDE)
        gate = g_ref[:, c].astype(F32)
        sg_ref[:, c] = (0.5 * gate * (1.0 + jnp.tanh(0.5 * gate)) * gain_ref[:, c]).astype(BF)
        rate = decay_rate(w_ref[:, c])
        cum = mm(upto, rate)
        before = mm(prior, rate)
        r = r_ref[:, c]
        k = k_ref[:, c]
        v = centred(v_ref[:, c])
        mid0, end0, mid1 = cum[63:64], cum[127:128], cum[191:192]
        r0 = r[:BLOCK] * jnp.exp2(before[:BLOCK] - mid0).astype(BF)
        k0 = k[:BLOCK] * jnp.exp2(mid0 - cum[:BLOCK]).astype(BF)
        r1 = r[BLOCK:] * jnp.exp2(before[BLOCK:] - mid1).astype(BF)
        k1 = k[BLOCK:] * jnp.exp2(mid1 - cum[BLOCK:]).astype(BF)
        r1c = r[BLOCK:] * jnp.exp2(before[BLOCK:] - end0).astype(BF)
        k0c = k[:BLOCK] * jnp.exp2(end0 - cum[:BLOCK]).astype(BF)
        rin_ref[:BLOCK, c] = r[:BLOCK] * jnp.exp2(before[:BLOCK]).astype(BF)
        rin_ref[BLOCK:, c] = r[BLOCK:] * jnp.exp2(before[BLOCK:]).astype(BF)
        heads = range(at // HALF, (at + WIDE) // HALF)
        u = jnp.concatenate([u_ref[h : h + 1] for h in heads], axis=1)
        bonus = (r.astype(F32) * u * k.astype(F32)).astype(BF)
        own = mm(bonus, head_ones(1.0)) * v.astype(F32)
        for p in range(WIDE // PAIR):
            s = slice(p * PAIR, (p + 1) * PAIR)
            o = slice(at + p * PAIR, at + (p + 1) * PAIR)
            s00 = side(mm_nt(stacked(r0[:, s]), k0[:, s]), True)
            s10 = side(mm_nt(stacked(r1c[:, s]), k0c[:, s]), False)
            s11 = side(mm_nt(stacked(r1[:, s]), k1[:, s]), True)
            v0, v1 = stacked(v[:BLOCK, s]), stacked(v[BLOCK:, s])
            out_ref[:BLOCK, o] = (mm(s00, v0) + own[:BLOCK, s]).astype(BF)
            out_ref[BLOCK:, o] = (mm(s10, v0) + mm(s11, v1) + own[BLOCK:, s]).astype(BF)

    for i in range(chunks):
        for one in load(i):
            one.wait()
        for part in range(i * wide // WIDE, (i + 1) * wide // WIDE):
            compute(part)
        for one in store(i):
            one.start()
    for i in range(chunks):
        for one in store(i):
            one.wait()


def scan_kernel(msg_ref, after_ref, out_ref):
    groups = msg_ref.shape[0]
    state = jnp.zeros((8, PAIR), F32)
    for g in range(groups):
        logs = msg_ref[g, 4].astype(F32)
        out_ref[g] = state.astype(BF)
        decay = jnp.exp2(logs[0:1] + logs[1:2])
        state = state * decay + msg_ref[g, 0:4].reshape(8, PAIR).astype(F32)


def finish_kernel(
    c_ref,
    s_ref,
    mine_out,
    mine_rin,
    mine_sg,
    other_out,
    other_rin,
    other_sg,
    w1_hbm,
    w2_hbm,
    y_hbm,
    out_buf,
    rin_buf,
    sg_buf,
    w_buf,
    wkv_buf,
    entering,
    gated,
    y_buf,
    in_sems,
    w_sems,
    y_sems,
):
    chunks = in_sems.shape[2]
    tiles = y_sems.shape[0]
    half = out_buf.shape[2]
    wide = half // chunks
    tile = y_buf.shape[1] // tiles
    parts = half // WIDE
    per = parts // chunks
    sources = ((mine_out, mine_rin, mine_sg), (other_out, other_rin, other_sg))
    buffers = (out_buf, rin_buf, sg_buf)

    def load(side, i):
        at = pl.ds(i * wide, wide)
        return [
            pltpu.make_async_copy(src.at[:, at], dst.at[side, :, at], in_sems.at[j, side, i])
            for j, (src, dst) in enumerate(zip(sources[side], buffers))
        ]

    def cols(t):
        return pl.ds(pl.multiple_of(t * tile, tile), tile)

    def fetch(j, t):
        src = (w1_hbm, w2_hbm)[j]
        return pltpu.make_async_copy(src.at[:, cols(t)], w_buf.at[j, :, cols(t)], w_sems.at[j, t])

    def store(t):
        return pltpu.make_async_copy(y_buf.at[:, cols(t)], y_hbm.at[:, cols(t)], y_sems.at[t])

    for side in range(2):
        for i in range(chunks):
            for one in load(side, i):
                one.start()
    first = lax.broadcasted_iota(jnp.int32, (HALF, PAIR), 1) < HALF
    zero = jnp.zeros((HALF, PAIR), BF)
    share = head_ones(1.0 / HALF)
    for side in range(2):
        base = (c_ref[0] if side == 0 else 1 - c_ref[0]) * (half // PAIR)
        for part in range(parts):
            for p in range(2):
                pair = s_ref[base + 2 * part + p]
                lanes = slice(p * PAIR, (p + 1) * PAIR)
                rest = slice((1 - p) * PAIR, (2 - p) * PAIR)
                low, high = p * PAIR, p * PAIR + HALF
                entering[side, part, low:high, lanes] = jnp.where(first, pair, zero)
                entering[side, part, high : low + PAIR, lanes] = jnp.where(first, zero, pair)
                entering[side, part, low : low + PAIR, rest] = jnp.zeros((PAIR, PAIR), BF)
    for side in range(2):
        for i in range(chunks):
            for one in load(side, i):
                one.wait()
            for t in WEIGHT_STAGES[side * chunks + i]:
                fetch(0, t).start()
                fetch(1, t).start()
            for part in range(i * per, (i + 1) * per):
                c = slice(part * WIDE, (part + 1) * WIDE)
                across = mm_nt(rin_buf[side, :, c], entering[side, part])
                wkv = out_buf[side, :, c].astype(F32) + across
                wkv_buf[side, :, c] = wkv
                gated[side, :, c] = (wkv * wkv).astype(BF)
    for side in range(2):
        for part in range(parts):
            c = slice(part * WIDE, (part + 1) * WIDE)
            var = mm(gated[side, :, c], share)
            gated[side, :, c] = (
                wkv_buf[side, :, c] * lax.rsqrt(var + EPS) * sg_buf[side, :, c].astype(F32)
            ).astype(BF)

    def project(t, carry):
        fetch(0, t).wait()
        fetch(1, t).wait()

        @pl.when(t + TILES_AHEAD < tiles)
        def _():
            fetch(0, t + TILES_AHEAD).start()
            fetch(1, t + TILES_AHEAD).start()

        y = mm(gated[0], w_buf[0, :, cols(t)]) + mm(gated[1], w_buf[1, :, cols(t)])
        y_buf[:, cols(t)] = y.astype(BF)
        store(t).start()
        return carry

    lax.fori_loop(0, tiles, project, 0)
    for t in range(tiles):
        store(t).wait()


def params(limit=66_000_000):
    return pltpu.CompilerParams(vmem_limit_bytes=limit)


def in_hbm(x):
    return pltpu.with_memory_space_constraint(x, pltpu.HBM)


def call_state(k, v, w, groups):
    chunks = 2
    any_block = pl.BlockSpec(memory_space=pl.ANY)
    shape = (groups, 5, 2, PAIR)
    return pl.pallas_call(
        state_kernel,
        in_specs=[any_block] * 3,
        out_specs=any_block,
        out_shape=jax.ShapeDtypeStruct(shape, BF),
        scratch_shapes=[pltpu.VMEM(k.shape, BF)] * 3
        + [
            pltpu.VMEM(shape, BF),
            pltpu.SemaphoreType.DMA((3, chunks)),
            pltpu.SemaphoreType.DMA((chunks,)),
        ],
        compiler_params=params(),
        cost_estimate=pl.CostEstimate(flops=4 << 30, bytes_accessed=4 << 20, transcendentals=1 << 20),
        name="state",
    )(k, v, w)


def call_local(side, r, k, v, w, g, bonus, gain):
    tokens, half = r.shape[0], gain.shape[1]
    chunks = 2
    any_block = pl.BlockSpec(memory_space=pl.ANY)
    vmem_block = pl.BlockSpec(memory_space=pltpu.VMEM)
    block = (tokens, half)
    return pl.pallas_call(
        local_kernel,
        in_specs=[pl.BlockSpec(memory_space=pltpu.SMEM)] + [vmem_block] * 2 + [any_block] * 5,
        out_specs=[any_block] * 3,
        out_shape=[pltpu.HBM(block, BF)] * 3,
        scratch_shapes=[pltpu.VMEM(block, BF)] * 8
        + [pltpu.SemaphoreType.DMA((5, chunks)), pltpu.SemaphoreType.DMA((3, chunks))],
        compiler_params=params(limit=32 << 20),
        cost_estimate=pl.CostEstimate(flops=8 << 30, bytes_accessed=4 << 20, transcendentals=2 << 20),
        name="local",
    )(side, bonus, gain, r, k, v, w, g)


def call_scan(msg, anchor):
    anchor = in_hbm(anchor)
    return pl.pallas_call(
        scan_kernel,
        in_specs=[pl.BlockSpec(memory_space=pltpu.VMEM), pl.BlockSpec(memory_space=pl.ANY)],
        out_shape=jax.ShapeDtypeStruct((msg.shape[0], 8, PAIR), BF),
        compiler_params=params(limit=8 << 20),
        name="scan",
    )(msg, anchor)


def call_finish(core, entering, mine, other, weight, other_weight):
    half, cols = weight.shape
    tokens = mine[0].shape[0]
    chunks, tiles = 2, 8
    mine, other = ([in_hbm(x) for x in part] for part in (mine, other))
    any_block = pl.BlockSpec(memory_space=pl.ANY)
    return pl.pallas_call(
        finish_kernel,
        in_specs=[pl.BlockSpec(memory_space=pltpu.SMEM), pl.BlockSpec(memory_space=pltpu.VMEM)]
        + [any_block] * 8,
        out_specs=any_block,
        out_shape=jax.ShapeDtypeStruct((tokens, cols), BF),
        scratch_shapes=[
            pltpu.VMEM((2, tokens, half), BF),
            pltpu.VMEM((2, tokens, half), BF),
            pltpu.VMEM((2, tokens, half), BF),
            pltpu.VMEM((2, half, cols), BF),
            pltpu.VMEM((2, tokens, half), F32),
            pltpu.VMEM((2, half // WIDE, WIDE, WIDE), BF),
            pltpu.VMEM((2, tokens, half), BF),
            pltpu.VMEM((tokens, cols), BF),
            pltpu.SemaphoreType.DMA((3, 2, chunks)),
            pltpu.SemaphoreType.DMA((2, tiles)),
            pltpu.SemaphoreType.DMA((tiles,)),
        ],
        compiler_params=params(limit=32 << 20),
        name="finish",
    )(core, entering, *mine, *other, in_hbm(weight), in_hbm(other_weight))


def shards(r, k, v, w, g, bonus, gain, weight):
    groups = lax.axis_size(SEQ_HEAD)
    core = lax.axis_index("head").reshape(1).astype(jnp.int32)
    r, k, v, w, g = (in_hbm(x) for x in (r, k, v, w, g))
    gain = gain.reshape(1, -1)
    swap = [(0, 1), (1, 0)]
    other_weight = lax.ppermute(weight, "head", swap)
    msg = call_state(k, v, w, groups)
    msg = lax.all_to_all(msg, SEQ_HEAD, split_axis=0, concat_axis=0, tiled=True)
    mine = call_local(core, r, k, v, w, g, bonus, gain)
    entering = call_scan(msg, mine[1])
    entering = lax.all_to_all(entering, SEQ_HEAD, split_axis=0, concat_axis=0, tiled=True)
    _, bonus, gain = lax.optimization_barrier((mine[1], bonus, gain))
    bonus, gain = (lax.ppermute(x, "head", swap) for x in (bonus, gain))
    other = call_local(1 - core, r, k, v, w, g, bonus, gain)
    entering = entering.reshape(-1, HALF, PAIR)
    return call_finish(core, entering, mine, other, weight, other_weight)


def solution(mesh):
    torus = Mesh(mesh.devices.reshape(4, 4, 4, mesh.shape["head"]), SEQ_HEAD)
    in_specs = (P(SEQ_HEAD, None),) * 5 + (P("head", None), P("head"), P("head", None))
    return jax.shard_map(
        shards, mesh=torus, in_specs=in_specs, out_specs=P(SEQ_HEAD, None), check_vma=False
    )
```

```python
import jax
import jax.numpy as jnp
from jax import lax
from jax.experimental import pallas as pl
from jax.experimental.pallas import tpu as pltpu
from jax.sharding import Mesh
from jax.sharding import PartitionSpec as P


BLOCK = 128
HALF = 64
PAIR = 128
WIDE = 256
SEQ_HEAD = ("seq_0", "seq_1", "seq_2", "head")
EPS = 1e-05
LOG2E = 1.4426950408889634
LOG2LOG2E = 0.5287663729448977
TILES_AHEAD = 4
BF = jnp.bfloat16
F32 = jnp.float32


def mm(a, b):
    return lax.dot_general(a, b, (((1,), (0,)), ((), ())), preferred_element_type=F32)


def mm_nt(a, b):
    return lax.dot_general(a, b, (((1,), (1,)), ((), ())), preferred_element_type=F32)


def mm_tn(a, b):
    return lax.dot_general(a, b, (((0,), (0,)), ((), ())), preferred_element_type=F32)


def grid2(rows, cols):
    return (
        lax.broadcasted_iota(jnp.int32, (rows, cols), 0),
        lax.broadcasted_iota(jnp.int32, (rows, cols), 1),
    )


def two_parts(x):
    hi = x.astype(BF)
    return hi, (x - hi.astype(F32)).astype(BF)


def head_ones(scale):
    row, col = grid2(WIDE, WIDE)
    return jnp.where(row // HALF == col // HALF, scale, 0.0).astype(BF)


def decay_rate(w):
    return jnp.exp2(w.astype(F32) * LOG2E + LOG2LOG2E).astype(BF)


def centred(v):
    return (v.astype(F32) - mm(v, head_ones(1.0 / HALF))).astype(BF)


def state_kernel(k_hbm, v_hbm, w_hbm, msg_hbm, k_buf, v_buf, w_buf, msg_buf, in_sems, out_sems):
    tokens, width = k_buf.shape
    chunks = in_sems.shape[1]
    wide = width // chunks
    per = msg_buf.shape[0] // chunks
    loads = [
        [
            pltpu.make_async_copy(
                src.at[:, pl.ds(i * wide, wide)], dst.at[:, pl.ds(i * wide, wide)], in_sems.at[j, i]
            )
            for j, (src, dst) in enumerate(((w_hbm, w_buf), (k_hbm, k_buf), (v_hbm, v_buf)))
        ]
        for i in range(chunks)
    ]
    stores = [
        pltpu.make_async_copy(
            msg_buf.at[pl.ds(i * per, per)], msg_hbm.at[pl.ds(i * per, per)], out_sems.at[i]
        )
        for i in range(chunks)
    ]
    depth = chunks
    for chunk in loads[:depth]:
        for one in chunk:
            one.start()
    row, col = grid2(tokens, tokens)
    later = jnp.where(col > row, -1.0, 0.0).astype(BF)
    first = lax.broadcasted_iota(jnp.int32, (HALF, PAIR), 1) < HALF
    for i in range(chunks):
        for one in loads[i]:
            one.wait()
        for one in loads[i + depth] if i + depth < chunks else ():
            one.start()
        for part in range(i * wide // WIDE, (i + 1) * wide // WIDE):
            s = slice(part * WIDE, (part + 1) * WIDE)
            rate = decay_rate(w_buf[:, s])
            after = mm(later, rate)
            key_end = k_buf[:, s] * jnp.exp2(after).astype(BF)
            total = after[0:1] - rate[0:1].astype(F32)
            state = mm_tn(v_buf[:, s], key_end)
            tot_hi, tot_lo = two_parts(total)
            logs = jnp.concatenate([tot_hi, tot_lo], axis=0)
            for p in range(WIDE // PAIR):
                at = p * PAIR
                both = jnp.where(
                    first,
                    state[at : at + HALF, at : at + PAIR],
                    state[at + HALF : at + PAIR, at : at + PAIR],
                )
                both = (both - jnp.mean(both, axis=0, keepdims=True)).astype(BF)
                base = (part * (WIDE // PAIR) + p) * 8
                msg_buf[base : base + 8, 0:4] = both.reshape(8, 4, 2, PAIR)
                msg_buf[base : base + 8, 4] = jnp.broadcast_to(
                    logs[None, :, at : at + PAIR], (8, 2, PAIR)
                )
        stores[i].start()
    for one in stores:
        one.wait()


def local_kernel(
    h_ref,
    u_ref,
    gain_ref,
    r_hbm,
    k_hbm,
    v_hbm,
    w_hbm,
    g_hbm,
    out_ref,
    rin_ref,
    sg_ref,
    r_ref,
    k_ref,
    v_ref,
    w_ref,
    g_ref,
    in_sems,
):
    tokens, half = r_ref.shape
    chunks = in_sems.shape[1]
    wide = half // chunks
    sources = (w_hbm, g_hbm, r_hbm, k_hbm, v_hbm)
    buffers = (w_ref, g_ref, r_ref, k_ref, v_ref)

    def load(i):
        at = pl.ds(pl.multiple_of(h_ref[0] * half + i * wide, wide), wide)
        to = pl.ds(i * wide, wide)
        return [
            pltpu.make_async_copy(src.at[:, at], dst.at[:, to], in_sems.at[j, i])
            for j, (src, dst) in enumerate(zip(sources, buffers))
        ]

    for i in range(chunks):
        for one in load(i):
            one.start()
    row, col = grid2(tokens, tokens)
    upto = jnp.where(col <= row, -1.0, 0.0).astype(BF)
    prior = jnp.where(col < row, -1.0, 0.0).astype(BF)
    lane = lax.broadcasted_iota(jnp.int32, (BLOCK, PAIR), 1)
    first = lane < HALF
    zero = jnp.zeros((BLOCK, PAIR), BF)
    row, col = grid2(BLOCK, BLOCK)
    strict = row > col

    def stacked(x):
        return jnp.concatenate([jnp.where(first, x, zero), jnp.where(first, zero, x)], axis=0)

    def side(scores, masked):
        a, b = scores[:BLOCK], scores[BLOCK:]
        if masked:
            a, b = jnp.where(strict, a, 0.0), jnp.where(strict, b, 0.0)
        return jnp.concatenate([a, b], axis=1).astype(BF)

    def compute(part):
        at = part * WIDE
        c = slice(at, at + WIDE)
        gate = g_ref[:, c].astype(F32)
        sg_ref[:, c] = (0.5 * gate * (1.0 + jnp.tanh(0.5 * gate)) * gain_ref[:, c]).astype(BF)
        rate = decay_rate(w_ref[:, c])
        cum = mm(upto, rate)
        before = mm(prior, rate)
        r = r_ref[:, c]
        k = k_ref[:, c]
        v = centred(v_ref[:, c])
        mid0, end0, mid1 = cum[63:64], cum[127:128], cum[191:192]
        r0 = r[:BLOCK] * jnp.exp2(before[:BLOCK] - mid0).astype(BF)
        k0 = k[:BLOCK] * jnp.exp2(mid0 - cum[:BLOCK]).astype(BF)
        r1 = r[BLOCK:] * jnp.exp2(before[BLOCK:] - mid1).astype(BF)
        k1 = k[BLOCK:] * jnp.exp2(mid1 - cum[BLOCK:]).astype(BF)
        r1c = r[BLOCK:] * jnp.exp2(before[BLOCK:] - end0).astype(BF)
        k0c = k[:BLOCK] * jnp.exp2(end0 - cum[:BLOCK]).astype(BF)
        rin_ref[:BLOCK, c] = r[:BLOCK] * jnp.exp2(before[:BLOCK]).astype(BF)
        rin_ref[BLOCK:, c] = r[BLOCK:] * jnp.exp2(before[BLOCK:]).astype(BF)
        heads = range(at // HALF, (at + WIDE) // HALF)
        u = jnp.concatenate([u_ref[h : h + 1] for h in heads], axis=1)
        bonus = (r.astype(F32) * u * k.astype(F32)).astype(BF)
        own = mm(bonus, head_ones(1.0)) * v.astype(F32)
        for p in range(WIDE // PAIR):
            s = slice(p * PAIR, (p + 1) * PAIR)
            o = slice(at + p * PAIR, at + (p + 1) * PAIR)
            s00 = side(mm_nt(stacked(r0[:, s]), k0[:, s]), True)
            s10 = side(mm_nt(stacked(r1c[:, s]), k0c[:, s]), False)
            s11 = side(mm_nt(stacked(r1[:, s]), k1[:, s]), True)
            v0, v1 = stacked(v[:BLOCK, s]), stacked(v[BLOCK:, s])
            out_ref[:BLOCK, o] = (mm(s00, v0) + own[:BLOCK, s]).astype(BF)
            out_ref[BLOCK:, o] = (mm(s10, v0) + mm(s11, v1) + own[BLOCK:, s]).astype(BF)

    for i in range(chunks):
        for one in load(i):
            one.wait()
        for part in range(i * wide // WIDE, (i + 1) * wide // WIDE):
            compute(part)


def scan_kernel(msg_ref, after_ref, out_ref):
    groups = msg_ref.shape[0]
    state = jnp.zeros((8, PAIR), F32)
    for g in range(groups):
        logs = msg_ref[g, 4].astype(F32)
        out_ref[g] = state.astype(BF)
        decay = jnp.exp2(logs[0:1] + logs[1:2])
        state = state * decay + msg_ref[g, 0:4].reshape(8, PAIR).astype(F32)


def finish_kernel(
    c_ref,
    s_ref,
    mine_out,
    mine_rin,
    mine_sg,
    other_out,
    other_rin,
    other_sg,
    w1_hbm,
    w2_hbm,
    y_hbm,
    w_buf,
    wkv_buf,
    entering,
    gated,
    y_buf,
    w_sems,
    y_sems,
):
    tiles = y_sems.shape[0]
    half = mine_out.shape[1]
    tile = y_buf.shape[1] // tiles
    parts = half // WIDE
    results = ((mine_out, mine_rin, mine_sg), (other_out, other_rin, other_sg))

    def cols(t):
        return pl.ds(pl.multiple_of(t * tile, tile), tile)

    def fetch(j, t):
        src = (w1_hbm, w2_hbm)[j]
        return pltpu.make_async_copy(src.at[:, cols(t)], w_buf.at[j, :, cols(t)], w_sems.at[j, t])

    def store(t):
        return pltpu.make_async_copy(y_buf.at[:, cols(t)], y_hbm.at[:, cols(t)], y_sems.at[t])

    for t in range(TILES_AHEAD):
        fetch(0, t).start()
        fetch(1, t).start()
    first = lax.broadcasted_iota(jnp.int32, (HALF, PAIR), 1) < HALF
    zero = jnp.zeros((HALF, PAIR), BF)
    share = head_ones(1.0 / HALF)
    for side in range(2):
        base = (c_ref[0] if side == 0 else 1 - c_ref[0]) * (half // PAIR)
        for part in range(parts):
            for p in range(2):
                pair = s_ref[base + 2 * part + p]
                lanes = slice(p * PAIR, (p + 1) * PAIR)
                rest = slice((1 - p) * PAIR, (2 - p) * PAIR)
                low, high = p * PAIR, p * PAIR + HALF
                entering[side, part, low:high, lanes] = jnp.where(first, pair, zero)
                entering[side, part, high : low + PAIR, lanes] = jnp.where(first, zero, pair)
                entering[side, part, low : low + PAIR, rest] = jnp.zeros((PAIR, PAIR), BF)
    for side in range(2):
        out_ref, rin_ref, _ = results[side]
        for part in range(parts):
            c = slice(part * WIDE, (part + 1) * WIDE)
            across = mm_nt(rin_ref[:, c], entering[side, part])
            wkv = out_ref[:, c].astype(F32) + across
            wkv_buf[side, :, c] = wkv
            gated[side, :, c] = (wkv * wkv).astype(BF)
    for side in range(2):
        sg_ref = results[side][2]
        for part in range(parts):
            c = slice(part * WIDE, (part + 1) * WIDE)
            var = mm(gated[side, :, c], share)
            gated[side, :, c] = (
                wkv_buf[side, :, c] * lax.rsqrt(var + EPS) * sg_ref[:, c].astype(F32)
            ).astype(BF)

    def project(t, carry):
        fetch(0, t).wait()
        fetch(1, t).wait()

        @pl.when(t + TILES_AHEAD < tiles)
        def _():
            fetch(0, t + TILES_AHEAD).start()
            fetch(1, t + TILES_AHEAD).start()

        y = mm(gated[0], w_buf[0, :, cols(t)]) + mm(gated[1], w_buf[1, :, cols(t)])
        y_buf[:, cols(t)] = y.astype(BF)
        store(t).start()
        return carry

    lax.fori_loop(0, tiles, project, 0)
    for t in range(tiles):
        store(t).wait()


def params(limit=66_000_000):
    return pltpu.CompilerParams(vmem_limit_bytes=limit)


def in_hbm(x):
    return pltpu.with_memory_space_constraint(x, pltpu.HBM)


def call_state(k, v, w, groups):
    chunks = 2
    any_block = pl.BlockSpec(memory_space=pl.ANY)
    shape = (groups, 5, 2, PAIR)
    return pl.pallas_call(
        state_kernel,
        in_specs=[any_block] * 3,
        out_specs=any_block,
        out_shape=jax.ShapeDtypeStruct(shape, BF),
        scratch_shapes=[pltpu.VMEM(k.shape, BF)] * 3
        + [
            pltpu.VMEM(shape, BF),
            pltpu.SemaphoreType.DMA((3, chunks)),
            pltpu.SemaphoreType.DMA((chunks,)),
        ],
        compiler_params=params(),
        cost_estimate=pl.CostEstimate(flops=4 << 30, bytes_accessed=4 << 20, transcendentals=1 << 20),
        name="state",
    )(k, v, w)


def call_local(side, r, k, v, w, g, bonus, gain):
    tokens, half = r.shape[0], gain.shape[1]
    chunks = 2
    any_block = pl.BlockSpec(memory_space=pl.ANY)
    vmem_block = pl.BlockSpec(memory_space=pltpu.VMEM)
    block = (tokens, half)
    return pl.pallas_call(
        local_kernel,
        in_specs=[pl.BlockSpec(memory_space=pltpu.SMEM)] + [vmem_block] * 2 + [any_block] * 5,
        out_specs=[vmem_block] * 3,
        out_shape=[jax.ShapeDtypeStruct(block, BF)] * 3,
        scratch_shapes=[pltpu.VMEM(block, BF)] * 5 + [pltpu.SemaphoreType.DMA((5, chunks))],
        compiler_params=params(limit=32 << 20),
        cost_estimate=pl.CostEstimate(flops=8 << 30, bytes_accessed=4 << 20, transcendentals=2 << 20),
        name="local",
    )(side, bonus, gain, r, k, v, w, g)


def call_scan(msg, anchor):
    return pl.pallas_call(
        scan_kernel,
        in_specs=[pl.BlockSpec(memory_space=pltpu.VMEM), pl.BlockSpec(memory_space=pl.ANY)],
        out_shape=jax.ShapeDtypeStruct((msg.shape[0], 8, PAIR), BF),
        compiler_params=params(limit=8 << 20),
        name="scan",
    )(msg, anchor)


def call_finish(core, entering, mine, other, weight, other_weight):
    half, cols = weight.shape
    tokens = mine[0].shape[0]
    tiles = 8
    any_block = pl.BlockSpec(memory_space=pl.ANY)
    return pl.pallas_call(
        finish_kernel,
        in_specs=[pl.BlockSpec(memory_space=pltpu.SMEM)]
        + [pl.BlockSpec(memory_space=pltpu.VMEM)] * 7
        + [any_block] * 2,
        out_specs=any_block,
        out_shape=jax.ShapeDtypeStruct((tokens, cols), BF),
        scratch_shapes=[
            pltpu.VMEM((2, half, cols), BF),
            pltpu.VMEM((2, tokens, half), F32),
            pltpu.VMEM((2, half // WIDE, WIDE, WIDE), BF),
            pltpu.VMEM((2, tokens, half), BF),
            pltpu.VMEM((tokens, cols), BF),
            pltpu.SemaphoreType.DMA((2, tiles)),
            pltpu.SemaphoreType.DMA((tiles,)),
        ],
        compiler_params=params(limit=32 << 20),
        name="finish",
    )(core, entering, *mine, *other, in_hbm(weight), in_hbm(other_weight))


def shards(r, k, v, w, g, bonus, gain, weight):
    groups = lax.axis_size(SEQ_HEAD)
    core = lax.axis_index("head").reshape(1).astype(jnp.int32)
    r, k, v, w, g = (in_hbm(x) for x in (r, k, v, w, g))
    gain = gain.reshape(1, -1)
    swap = [(0, 1), (1, 0)]
    other_weight = lax.ppermute(weight, "head", swap)
    msg = call_state(k, v, w, groups)
    msg = lax.all_to_all(msg, SEQ_HEAD, split_axis=0, concat_axis=0, tiled=True)
    mine = call_local(core, r, k, v, w, g, bonus, gain)
    entering = call_scan(msg, mine[1])
    entering = lax.all_to_all(entering, SEQ_HEAD, split_axis=0, concat_axis=0, tiled=True)
    _, bonus, gain = lax.optimization_barrier((mine[1], bonus, gain))
    bonus, gain = (lax.ppermute(x, "head", swap) for x in (bonus, gain))
    other = call_local(1 - core, r, k, v, w, g, bonus, gain)
    entering = entering.reshape(-1, HALF, PAIR)
    return call_finish(core, entering, mine, other, weight, other_weight)


def solution(mesh):
    torus = Mesh(mesh.devices.reshape(4, 4, 4, mesh.shape["head"]), SEQ_HEAD)
    in_specs = (P(SEQ_HEAD, None),) * 5 + (P("head", None), P("head"), P("head", None))
    return jax.shard_map(
        shards, mesh=torus, in_specs=in_specs, out_specs=P(SEQ_HEAD, None), check_vma=False
    )
```

```python
import jax
import jax.numpy as jnp
from jax import lax
from jax.experimental import pallas as pl
from jax.experimental.pallas import tpu as pltpu
from jax.sharding import Mesh
from jax.sharding import PartitionSpec as P


BLOCK = 128
HALF = 64
PAIR = 128
WIDE = 256
SEQ_HEAD = ("seq_0", "seq_1", "seq_2", "head")
EPS = 1e-05
LOG2E = 1.4426950408889634
LOG2LOG2E = 0.5287663729448977
TILES_AHEAD = 4
BF = jnp.bfloat16
F32 = jnp.float32


def mm(a, b):
    return lax.dot_general(a, b, (((1,), (0,)), ((), ())), preferred_element_type=F32)


def mm_nt(a, b):
    return lax.dot_general(a, b, (((1,), (1,)), ((), ())), preferred_element_type=F32)


def mm_tn(a, b):
    return lax.dot_general(a, b, (((0,), (0,)), ((), ())), preferred_element_type=F32)


def grid2(rows, cols):
    return (
        lax.broadcasted_iota(jnp.int32, (rows, cols), 0),
        lax.broadcasted_iota(jnp.int32, (rows, cols), 1),
    )


def two_parts(x):
    hi = x.astype(BF)
    return hi, (x - hi.astype(F32)).astype(BF)


def head_ones(scale):
    row, col = grid2(WIDE, WIDE)
    return jnp.where(row // HALF == col // HALF, scale, 0.0).astype(BF)


def decay_rate(w):
    return jnp.exp2(w.astype(F32) * LOG2E + LOG2LOG2E).astype(BF)


def centred(v):
    row, col = grid2(WIDE, WIDE)
    less_mean = jnp.where(row == col, 1.0, 0.0) - jnp.where(row // HALF == col // HALF, 1.0 / HALF, 0.0)
    return mm(v, less_mean.astype(BF)).astype(BF)


def state_kernel(k_hbm, v_hbm, w_hbm, msg_hbm, k_buf, v_buf, w_buf, msg_buf, in_sems, out_sems):
    tokens, width = k_buf.shape
    chunks = in_sems.shape[1]
    wide = width // chunks
    per = msg_buf.shape[0] // chunks
    loads = [
        [
            pltpu.make_async_copy(
                src.at[:, pl.ds(i * wide, wide)], dst.at[:, pl.ds(i * wide, wide)], in_sems.at[j, i]
            )
            for j, (src, dst) in enumerate(((w_hbm, w_buf), (k_hbm, k_buf), (v_hbm, v_buf)))
        ]
        for i in range(chunks)
    ]
    stores = [
        pltpu.make_async_copy(
            msg_buf.at[pl.ds(i * per, per)], msg_hbm.at[pl.ds(i * per, per)], out_sems.at[i]
        )
        for i in range(chunks)
    ]
    depth = chunks
    for chunk in loads[:depth]:
        for one in chunk:
            one.start()
    row, col = grid2(tokens, tokens)
    later = jnp.where(col > row, -1.0, 0.0).astype(BF)
    first = lax.broadcasted_iota(jnp.int32, (HALF, PAIR), 1) < HALF
    for i in range(chunks):
        for one in loads[i]:
            one.wait()
        for one in loads[i + depth] if i + depth < chunks else ():
            one.start()
        for part in range(i * wide // WIDE, (i + 1) * wide // WIDE):
            s = slice(part * WIDE, (part + 1) * WIDE)
            rate = decay_rate(w_buf[:, s])
            after = mm(later, rate)
            key_end = (k_buf[:, s].astype(F32) * jnp.exp2(after)).astype(BF)
            total = after[0:1] - rate[0:1].astype(F32)
            state = mm_tn(v_buf[:, s], key_end)
            tot_hi, tot_lo = two_parts(total)
            logs = jnp.concatenate([tot_hi, tot_lo], axis=0)
            for p in range(WIDE // PAIR):
                at = p * PAIR
                both = jnp.where(
                    first,
                    state[at : at + HALF, at : at + PAIR],
                    state[at + HALF : at + PAIR, at : at + PAIR],
                )
                both = (both - jnp.mean(both, axis=0, keepdims=True)).astype(BF)
                base = (part * (WIDE // PAIR) + p) * 8
                msg_buf[base : base + 8, 0:4] = both.reshape(8, 4, 2, PAIR)
                msg_buf[base : base + 8, 4] = jnp.broadcast_to(
                    logs[None, :, at : at + PAIR], (8, 2, PAIR)
                )
        stores[i].start()
    for one in stores:
        one.wait()


def local_kernel(
    h_ref,
    u_ref,
    gain_ref,
    r_hbm,
    k_hbm,
    v_hbm,
    w_hbm,
    g_hbm,
    out_ref,
    rin_ref,
    sg_ref,
    r_ref,
    k_ref,
    v_ref,
    w_ref,
    g_ref,
    in_sems,
):
    tokens, half = r_ref.shape
    chunks = in_sems.shape[1]
    wide = half // chunks
    sources = (w_hbm, g_hbm, r_hbm, k_hbm, v_hbm)
    buffers = (w_ref, g_ref, r_ref, k_ref, v_ref)

    def load(i):
        at = pl.ds(pl.multiple_of(h_ref[0] * half + i * wide, wide), wide)
        to = pl.ds(i * wide, wide)
        return [
            pltpu.make_async_copy(src.at[:, at], dst.at[:, to], in_sems.at[j, i])
            for j, (src, dst) in enumerate(zip(sources, buffers))
        ]

    for i in range(chunks):
        for one in load(i):
            one.start()
    row, col = grid2(tokens, tokens)
    upto = jnp.where(col <= row, -1.0, 0.0).astype(BF)
    prior = jnp.where(col < row, -1.0, 0.0).astype(BF)
    lane = lax.broadcasted_iota(jnp.int32, (BLOCK, PAIR), 1)
    first = lane < HALF
    zero = jnp.zeros((BLOCK, PAIR), BF)
    row, col = grid2(BLOCK, BLOCK)
    strict = row > col

    def stacked(x):
        return jnp.concatenate([jnp.where(first, x, zero), jnp.where(first, zero, x)], axis=0)

    def side(scores, masked):
        a, b = scores[:BLOCK], scores[BLOCK:]
        if masked:
            a, b = jnp.where(strict, a, 0.0), jnp.where(strict, b, 0.0)
        return jnp.concatenate([a, b], axis=1).astype(BF)

    def compute(part):
        at = part * WIDE
        c = slice(at, at + WIDE)
        gate = g_ref[:, c].astype(F32)
        sg_ref[:, c] = (0.5 * gate * (1.0 + jnp.tanh(0.5 * gate)) * gain_ref[:, c]).astype(BF)
        rate = decay_rate(w_ref[:, c])
        cum = mm(upto, rate)
        before = mm(prior, rate)
        r = r_ref[:, c]
        k = k_ref[:, c]
        v = centred(v_ref[:, c])
        mid0, end0, mid1 = cum[63:64], cum[127:128], cum[191:192]
        rf, kf = r.astype(F32), k.astype(F32)
        r0 = (rf[:BLOCK] * jnp.exp2(before[:BLOCK] - mid0)).astype(BF)
        k0 = (kf[:BLOCK] * jnp.exp2(mid0 - cum[:BLOCK])).astype(BF)
        r1 = (rf[BLOCK:] * jnp.exp2(before[BLOCK:] - mid1)).astype(BF)
        k1 = (kf[BLOCK:] * jnp.exp2(mid1 - cum[BLOCK:])).astype(BF)
        r1c = (rf[BLOCK:] * jnp.exp2(before[BLOCK:] - end0)).astype(BF)
        k0c = (kf[:BLOCK] * jnp.exp2(end0 - cum[:BLOCK])).astype(BF)
        rin_ref[:BLOCK, c] = (rf[:BLOCK] * jnp.exp2(before[:BLOCK])).astype(BF)
        rin_ref[BLOCK:, c] = (rf[BLOCK:] * jnp.exp2(before[BLOCK:])).astype(BF)
        heads = range(at // HALF, (at + WIDE) // HALF)
        u = jnp.concatenate([u_ref[h : h + 1] for h in heads], axis=1)
        bonus = (rf * u * kf).astype(BF)
        own = mm(bonus, head_ones(1.0)) * v.astype(F32)
        for p in range(WIDE // PAIR):
            s = slice(p * PAIR, (p + 1) * PAIR)
            o = slice(at + p * PAIR, at + (p + 1) * PAIR)
            s00 = side(mm_nt(stacked(r0[:, s]), k0[:, s]), True)
            s10 = side(mm_nt(stacked(r1c[:, s]), k0c[:, s]), False)
            s11 = side(mm_nt(stacked(r1[:, s]), k1[:, s]), True)
            v0, v1 = stacked(v[:BLOCK, s]), stacked(v[BLOCK:, s])
            out_ref[:BLOCK, o] = (mm(s00, v0) + own[:BLOCK, s]).astype(BF)
            out_ref[BLOCK:, o] = (mm(s10, v0) + mm(s11, v1) + own[BLOCK:, s]).astype(BF)

    for i in range(chunks):
        for one in load(i):
            one.wait()
        for part in range(i * wide // WIDE, (i + 1) * wide // WIDE):
            compute(part)


def scan_kernel(msg_ref, after_ref, out_ref):
    groups = msg_ref.shape[0]
    state = jnp.zeros((8, PAIR), F32)
    for g in range(groups):
        logs = msg_ref[g, 4].astype(F32)
        out_ref[g] = state.astype(BF)
        decay = jnp.exp2(logs[0:1] + logs[1:2])
        state = state * decay + msg_ref[g, 0:4].reshape(8, PAIR).astype(F32)


def finish_kernel(
    c_ref,
    s_ref,
    mine_out,
    mine_rin,
    mine_sg,
    other_out,
    other_rin,
    other_sg,
    w1_hbm,
    w2_hbm,
    y_hbm,
    w_buf,
    wkv_buf,
    entering,
    gated,
    y_buf,
    w_sems,
    y_sems,
):
    tiles = y_sems.shape[0]
    half = mine_out.shape[1]
    tile = y_buf.shape[1] // tiles
    parts = half // WIDE
    results = ((mine_out, mine_rin, mine_sg), (other_out, other_rin, other_sg))

    def cols(t):
        return pl.ds(pl.multiple_of(t * tile, tile), tile)

    def fetch(j, t):
        src = (w1_hbm, w2_hbm)[j]
        return pltpu.make_async_copy(src.at[:, cols(t)], w_buf.at[j, :, cols(t)], w_sems.at[j, t])

    def store(t):
        return pltpu.make_async_copy(y_buf.at[:, cols(t)], y_hbm.at[:, cols(t)], y_sems.at[t])

    for t in range(TILES_AHEAD):
        fetch(0, t).start()
        fetch(1, t).start()
    first = lax.broadcasted_iota(jnp.int32, (HALF, PAIR), 1) < HALF
    zero = jnp.zeros((HALF, PAIR), BF)
    share = head_ones(1.0 / HALF)
    for side in range(2):
        base = (c_ref[0] if side == 0 else 1 - c_ref[0]) * (half // PAIR)
        for part in range(parts):
            for p in range(2):
                pair = s_ref[base + 2 * part + p]
                lanes = slice(p * PAIR, (p + 1) * PAIR)
                rest = slice((1 - p) * PAIR, (2 - p) * PAIR)
                low, high = p * PAIR, p * PAIR + HALF
                entering[side, part, low:high, lanes] = jnp.where(first, pair, zero)
                entering[side, part, high : low + PAIR, lanes] = jnp.where(first, zero, pair)
                entering[side, part, low : low + PAIR, rest] = jnp.zeros((PAIR, PAIR), BF)
    for side in range(2):
        out_ref, rin_ref, _ = results[side]
        for part in range(parts):
            c = slice(part * WIDE, (part + 1) * WIDE)
            across = mm_nt(rin_ref[:, c], entering[side, part])
            wkv = out_ref[:, c].astype(F32) + across
            wkv_buf[side, :, c] = wkv
            gated[side, :, c] = (wkv * wkv).astype(BF)
    for side in range(2):
        sg_ref = results[side][2]
        for part in range(parts):
            c = slice(part * WIDE, (part + 1) * WIDE)
            var = mm(gated[side, :, c], share)
            gated[side, :, c] = (
                wkv_buf[side, :, c] * lax.rsqrt(var + EPS) * sg_ref[:, c].astype(F32)
            ).astype(BF)

    def project(t, carry):
        fetch(0, t).wait()
        fetch(1, t).wait()

        @pl.when(t + TILES_AHEAD < tiles)
        def _():
            fetch(0, t + TILES_AHEAD).start()
            fetch(1, t + TILES_AHEAD).start()

        y = mm(gated[0], w_buf[0, :, cols(t)]) + mm(gated[1], w_buf[1, :, cols(t)])
        y_buf[:, cols(t)] = y.astype(BF)
        store(t).start()
        return carry

    lax.fori_loop(0, tiles, project, 0)
    for t in range(tiles):
        store(t).wait()


def params(limit=66_000_000):
    return pltpu.CompilerParams(vmem_limit_bytes=limit)


def in_hbm(x):
    return pltpu.with_memory_space_constraint(x, pltpu.HBM)


def call_state(k, v, w, groups):
    chunks = 2
    any_block = pl.BlockSpec(memory_space=pl.ANY)
    shape = (groups, 5, 2, PAIR)
    return pl.pallas_call(
        state_kernel,
        in_specs=[any_block] * 3,
        out_specs=any_block,
        out_shape=jax.ShapeDtypeStruct(shape, BF),
        scratch_shapes=[pltpu.VMEM(k.shape, BF)] * 3
        + [
            pltpu.VMEM(shape, BF),
            pltpu.SemaphoreType.DMA((3, chunks)),
            pltpu.SemaphoreType.DMA((chunks,)),
        ],
        compiler_params=params(),
        cost_estimate=pl.CostEstimate(flops=4 << 30, bytes_accessed=4 << 20, transcendentals=1 << 20),
        name="state",
    )(k, v, w)


def call_local(side, r, k, v, w, g, bonus, gain):
    tokens, half = r.shape[0], gain.shape[1]
    chunks = 2
    any_block = pl.BlockSpec(memory_space=pl.ANY)
    vmem_block = pl.BlockSpec(memory_space=pltpu.VMEM)
    block = (tokens, half)
    return pl.pallas_call(
        local_kernel,
        in_specs=[pl.BlockSpec(memory_space=pltpu.SMEM)] + [vmem_block] * 2 + [any_block] * 5,
        out_specs=[vmem_block] * 3,
        out_shape=[jax.ShapeDtypeStruct(block, BF)] * 3,
        scratch_shapes=[pltpu.VMEM(block, BF)] * 5 + [pltpu.SemaphoreType.DMA((5, chunks))],
        compiler_params=params(limit=32 << 20),
        cost_estimate=pl.CostEstimate(flops=8 << 30, bytes_accessed=4 << 20, transcendentals=2 << 20),
        name="local",
    )(side, bonus, gain, r, k, v, w, g)


def call_scan(msg, anchor):
    return pl.pallas_call(
        scan_kernel,
        in_specs=[pl.BlockSpec(memory_space=pltpu.VMEM), pl.BlockSpec(memory_space=pl.ANY)],
        out_shape=jax.ShapeDtypeStruct((msg.shape[0], 8, PAIR), BF),
        compiler_params=params(limit=8 << 20),
        name="scan",
    )(msg, anchor)


def call_finish(core, entering, mine, other, weight, other_weight):
    half, cols = weight.shape
    tokens = mine[0].shape[0]
    tiles = 8
    any_block = pl.BlockSpec(memory_space=pl.ANY)
    return pl.pallas_call(
        finish_kernel,
        in_specs=[pl.BlockSpec(memory_space=pltpu.SMEM)]
        + [pl.BlockSpec(memory_space=pltpu.VMEM)] * 7
        + [any_block] * 2,
        out_specs=any_block,
        out_shape=jax.ShapeDtypeStruct((tokens, cols), BF),
        scratch_shapes=[
            pltpu.VMEM((2, half, cols), BF),
            pltpu.VMEM((2, tokens, half), F32),
            pltpu.VMEM((2, half // WIDE, WIDE, WIDE), BF),
            pltpu.VMEM((2, tokens, half), BF),
            pltpu.VMEM((tokens, cols), BF),
            pltpu.SemaphoreType.DMA((2, tiles)),
            pltpu.SemaphoreType.DMA((tiles,)),
        ],
        compiler_params=params(limit=32 << 20),
        name="finish",
    )(core, entering, *mine, *other, in_hbm(weight), in_hbm(other_weight))


def shards(r, k, v, w, g, bonus, gain, weight):
    groups = lax.axis_size(SEQ_HEAD)
    core = lax.axis_index("head").reshape(1).astype(jnp.int32)
    r, k, v, w, g = (in_hbm(x) for x in (r, k, v, w, g))
    gain = gain.reshape(1, -1)
    swap = [(0, 1), (1, 0)]
    other_weight = lax.ppermute(weight, "head", swap)
    msg = call_state(k, v, w, groups)
    msg = lax.all_to_all(msg, SEQ_HEAD, split_axis=0, concat_axis=0, tiled=True)
    mine = call_local(core, r, k, v, w, g, bonus, gain)
    entering = call_scan(msg, mine[1])
    entering = lax.all_to_all(entering, SEQ_HEAD, split_axis=0, concat_axis=0, tiled=True)
    _, bonus, gain = lax.optimization_barrier((mine[1], bonus, gain))
    bonus, gain = (lax.ppermute(x, "head", swap) for x in (bonus, gain))
    other = call_local(1 - core, r, k, v, w, g, bonus, gain)
    entering = entering.reshape(-1, HALF, PAIR)
    return call_finish(core, entering, mine, other, weight, other_weight)


def solution(mesh):
    torus = Mesh(mesh.devices.reshape(4, 4, 4, mesh.shape["head"]), SEQ_HEAD)
    in_specs = (P(SEQ_HEAD, None),) * 5 + (P("head", None), P("head"), P("head", None))
    return jax.shard_map(
        shards, mesh=torus, in_specs=in_specs, out_specs=P(SEQ_HEAD, None), check_vma=False
    )
```

```python
import jax
import jax.numpy as jnp
from jax import lax
from jax.experimental import pallas as pl
from jax.experimental.pallas import tpu as pltpu
from jax.sharding import Mesh
from jax.sharding import PartitionSpec as P


BLOCK = 128
HALF = 64
PAIR = 128
WIDE = 256
SEQ_HEAD = ("seq_0", "seq_1", "seq_2", "head")
EPS = 1e-05
LOG2E = 1.4426950408889634
LOG2LOG2E = 0.5287663729448977
TILES_AHEAD = 5
BF = jnp.bfloat16
F32 = jnp.float32


def mm(a, b):
    return lax.dot_general(a, b, (((1,), (0,)), ((), ())), preferred_element_type=F32)


def mm_nt(a, b):
    return lax.dot_general(a, b, (((1,), (1,)), ((), ())), preferred_element_type=F32)


def mm_tn(a, b):
    return lax.dot_general(a, b, (((0,), (0,)), ((), ())), preferred_element_type=F32)


def grid2(rows, cols):
    return (
        lax.broadcasted_iota(jnp.int32, (rows, cols), 0),
        lax.broadcasted_iota(jnp.int32, (rows, cols), 1),
    )


def two_parts(x):
    hi = x.astype(BF)
    return hi, (x - hi.astype(F32)).astype(BF)


def head_ones(scale):
    row, col = grid2(WIDE, WIDE)
    return jnp.where(row // HALF == col // HALF, scale, 0.0).astype(BF)


def decay_rate(w):
    return jnp.exp2(w.astype(F32) * LOG2E + LOG2LOG2E).astype(BF)


def centred(v):
    row, col = grid2(WIDE, WIDE)
    less_mean = jnp.where(row == col, 1.0, 0.0) - jnp.where(row // HALF == col // HALF, 1.0 / HALF, 0.0)
    return mm(v, less_mean.astype(BF)).astype(BF)


def state_kernel(k_hbm, v_hbm, w_hbm, msg_hbm, k_buf, v_buf, w_buf, msg_buf, in_sems, out_sems):
    tokens, width = k_buf.shape
    chunks = in_sems.shape[1]
    wide = width // chunks
    per = msg_buf.shape[0] // chunks
    loads = [
        [
            pltpu.make_async_copy(
                src.at[:, pl.ds(i * wide, wide)], dst.at[:, pl.ds(i * wide, wide)], in_sems.at[j, i]
            )
            for j, (src, dst) in enumerate(((w_hbm, w_buf), (k_hbm, k_buf), (v_hbm, v_buf)))
        ]
        for i in range(chunks)
    ]
    stores = [
        pltpu.make_async_copy(
            msg_buf.at[pl.ds(i * per, per)], msg_hbm.at[pl.ds(i * per, per)], out_sems.at[i]
        )
        for i in range(chunks)
    ]
    depth = chunks
    for chunk in loads[:depth]:
        for one in chunk:
            one.start()
    row, col = grid2(tokens, tokens)
    later = jnp.where(col > row, -1.0, 0.0).astype(BF)
    first = lax.broadcasted_iota(jnp.int32, (HALF, PAIR), 1) < HALF
    for i in range(chunks):
        for one in loads[i]:
            one.wait()
        for one in loads[i + depth] if i + depth < chunks else ():
            one.start()
        for part in range(i * wide // WIDE, (i + 1) * wide // WIDE):
            s = slice(part * WIDE, (part + 1) * WIDE)
            rate = decay_rate(w_buf[:, s])
            after = mm(later, rate)
            key_end = (k_buf[:, s].astype(F32) * jnp.exp2(after)).astype(BF)
            total = after[0:1] - rate[0:1].astype(F32)
            state = mm_tn(v_buf[:, s], key_end)
            tot_hi, tot_lo = two_parts(total)
            logs = jnp.concatenate([tot_hi, tot_lo], axis=0)
            for p in range(WIDE // PAIR):
                at = p * PAIR
                both = jnp.where(
                    first,
                    state[at : at + HALF, at : at + PAIR],
                    state[at + HALF : at + PAIR, at : at + PAIR],
                )
                both = (both - jnp.mean(both, axis=0, keepdims=True)).astype(BF)
                base = (part * (WIDE // PAIR) + p) * 8
                msg_buf[base : base + 8, 0:4] = both.reshape(8, 4, 2, PAIR)
                msg_buf[base : base + 8, 4] = jnp.broadcast_to(
                    logs[None, :, at : at + PAIR], (8, 2, PAIR)
                )
        stores[i].start()
    for one in stores:
        one.wait()


def local_kernel(
    h_ref,
    u_ref,
    gain_ref,
    r_hbm,
    k_hbm,
    v_hbm,
    w_hbm,
    g_hbm,
    out_ref,
    rin_ref,
    sg_ref,
    r_ref,
    k_ref,
    v_ref,
    w_ref,
    g_ref,
    in_sems,
):
    tokens, half = r_ref.shape
    chunks = in_sems.shape[1]
    wide = half // chunks
    sources = (w_hbm, g_hbm, r_hbm, k_hbm, v_hbm)
    buffers = (w_ref, g_ref, r_ref, k_ref, v_ref)

    def load(i):
        at = pl.ds(pl.multiple_of(h_ref[0] * half + i * wide, wide), wide)
        to = pl.ds(i * wide, wide)
        return [
            pltpu.make_async_copy(src.at[:, at], dst.at[:, to], in_sems.at[j, i])
            for j, (src, dst) in enumerate(zip(sources, buffers))
        ]

    for i in range(chunks):
        for one in load(i):
            one.start()
    row, col = grid2(tokens, tokens)
    upto = jnp.where(col <= row, -1.0, 0.0).astype(BF)
    prior = jnp.where(col < row, -1.0, 0.0).astype(BF)
    lane = lax.broadcasted_iota(jnp.int32, (BLOCK, PAIR), 1)
    first = lane < HALF
    zero = jnp.zeros((BLOCK, PAIR), BF)
    row, col = grid2(BLOCK, BLOCK)
    strict = row > col

    def stacked(x):
        return jnp.concatenate([jnp.where(first, x, zero), jnp.where(first, zero, x)], axis=0)

    def side(scores, masked):
        a, b = scores[:BLOCK], scores[BLOCK:]
        if masked:
            a, b = jnp.where(strict, a, 0.0), jnp.where(strict, b, 0.0)
        return jnp.concatenate([a, b], axis=1).astype(BF)

    def compute(part):
        at = part * WIDE
        c = slice(at, at + WIDE)
        gate = g_ref[:, c].astype(F32)
        sg_ref[:, c] = (0.5 * gate * (1.0 + jnp.tanh(0.5 * gate)) * gain_ref[:, c]).astype(BF)
        rate = decay_rate(w_ref[:, c])
        cum = mm(upto, rate)
        before = mm(prior, rate)
        r = r_ref[:, c]
        k = k_ref[:, c]
        v = centred(v_ref[:, c])
        mid0, end0, mid1 = cum[63:64], cum[127:128], cum[191:192]
        rf, kf = r.astype(F32), k.astype(F32)
        r0 = (rf[:BLOCK] * jnp.exp2(before[:BLOCK] - mid0)).astype(BF)
        k0 = (kf[:BLOCK] * jnp.exp2(mid0 - cum[:BLOCK])).astype(BF)
        r1 = (rf[BLOCK:] * jnp.exp2(before[BLOCK:] - mid1)).astype(BF)
        k1 = (kf[BLOCK:] * jnp.exp2(mid1 - cum[BLOCK:])).astype(BF)
        r1c = (rf[BLOCK:] * jnp.exp2(before[BLOCK:] - end0)).astype(BF)
        k0c = (kf[:BLOCK] * jnp.exp2(end0 - cum[:BLOCK])).astype(BF)
        rin_ref[:BLOCK, c] = (rf[:BLOCK] * jnp.exp2(before[:BLOCK])).astype(BF)
        rin_ref[BLOCK:, c] = (rf[BLOCK:] * jnp.exp2(before[BLOCK:])).astype(BF)
        heads = range(at // HALF, (at + WIDE) // HALF)
        u = jnp.concatenate([u_ref[h : h + 1] for h in heads], axis=1)
        bonus = (rf * u * kf).astype(BF)
        own = mm(bonus, head_ones(1.0)) * v.astype(F32)
        for p in range(WIDE // PAIR):
            s = slice(p * PAIR, (p + 1) * PAIR)
            o = slice(at + p * PAIR, at + (p + 1) * PAIR)
            s00 = side(mm_nt(stacked(r0[:, s]), k0[:, s]), True)
            s10 = side(mm_nt(stacked(r1c[:, s]), k0c[:, s]), False)
            s11 = side(mm_nt(stacked(r1[:, s]), k1[:, s]), True)
            v0, v1 = stacked(v[:BLOCK, s]), stacked(v[BLOCK:, s])
            out_ref[:BLOCK, o] = (mm(s00, v0) + own[:BLOCK, s]).astype(BF)
            out_ref[BLOCK:, o] = (mm(s10, v0) + mm(s11, v1) + own[BLOCK:, s]).astype(BF)

    for i in range(chunks):
        for one in load(i):
            one.wait()
        for part in range(i * wide // WIDE, (i + 1) * wide // WIDE):
            compute(part)


def scan_kernel(msg_ref, after_ref, out_hbm, out_ref, sems):
    groups = msg_ref.shape[0]
    pieces = sems.shape[0]
    per = groups // pieces
    stores = [
        pltpu.make_async_copy(out_ref.at[pl.ds(i * per, per)], out_hbm.at[pl.ds(i * per, per)], sems.at[i])
        for i in range(pieces)
    ]
    state = jnp.zeros((8, PAIR), F32)
    for g in range(groups):
        logs = msg_ref[g, 4].astype(F32)
        out_ref[g] = state.astype(BF)
        if g % per == per - 1:
            stores[g // per].start()
        decay = jnp.exp2(logs[0:1] + logs[1:2])
        state = state * decay + msg_ref[g, 0:4].reshape(8, PAIR).astype(F32)
    for one in stores:
        one.wait()


def finish_kernel(
    c_ref,
    s_ref,
    mine_out,
    mine_rin,
    mine_sg,
    other_out,
    other_rin,
    other_sg,
    w1_hbm,
    w2_hbm,
    y_hbm,
    w_buf,
    wkv_buf,
    entering,
    gated,
    y_buf,
    w_sems,
    y_sems,
):
    tiles = y_sems.shape[0]
    half = mine_out.shape[1]
    tile = y_buf.shape[1] // tiles
    parts = half // WIDE
    results = ((mine_out, mine_rin, mine_sg), (other_out, other_rin, other_sg))

    def cols(t):
        return pl.ds(pl.multiple_of(t * tile, tile), tile)

    def fetch(j, t):
        src = (w1_hbm, w2_hbm)[j]
        return pltpu.make_async_copy(src.at[:, cols(t)], w_buf.at[j, :, cols(t)], w_sems.at[j, t])

    def store(t):
        return pltpu.make_async_copy(y_buf.at[:, cols(t)], y_hbm.at[:, cols(t)], y_sems.at[t])

    for t in range(TILES_AHEAD):
        fetch(0, t).start()
        fetch(1, t).start()
    first = lax.broadcasted_iota(jnp.int32, (HALF, PAIR), 1) < HALF
    zero = jnp.zeros((HALF, PAIR), BF)
    share = head_ones(1.0 / HALF)
    for side in range(2):
        base = (c_ref[0] if side == 0 else 1 - c_ref[0]) * (half // PAIR)
        for part in range(parts):
            for p in range(2):
                pair = s_ref[base + 2 * part + p]
                lanes = slice(p * PAIR, (p + 1) * PAIR)
                rest = slice((1 - p) * PAIR, (2 - p) * PAIR)
                low, high = p * PAIR, p * PAIR + HALF
                entering[side, part, low:high, lanes] = jnp.where(first, pair, zero)
                entering[side, part, high : low + PAIR, lanes] = jnp.where(first, zero, pair)
                entering[side, part, low : low + PAIR, rest] = jnp.zeros((PAIR, PAIR), BF)
    for side in range(2):
        out_ref, rin_ref, _ = results[side]
        for part in range(parts):
            c = slice(part * WIDE, (part + 1) * WIDE)
            across = mm_nt(rin_ref[:, c], entering[side, part])
            wkv = out_ref[:, c].astype(F32) + across
            wkv_buf[side, :, c] = wkv
            gated[side, :, c] = (wkv * wkv).astype(BF)
    for side in range(2):
        sg_ref = results[side][2]
        for part in range(parts):
            c = slice(part * WIDE, (part + 1) * WIDE)
            var = mm(gated[side, :, c], share)
            gated[side, :, c] = (
                wkv_buf[side, :, c] * lax.rsqrt(var + EPS) * sg_ref[:, c].astype(F32)
            ).astype(BF)

    def project(t, carry):
        fetch(0, t).wait()
        fetch(1, t).wait()

        @pl.when(t + TILES_AHEAD < tiles)
        def _():
            fetch(0, t + TILES_AHEAD).start()
            fetch(1, t + TILES_AHEAD).start()

        y = mm(gated[0], w_buf[0, :, cols(t)]) + mm(gated[1], w_buf[1, :, cols(t)])
        y_buf[:, cols(t)] = y.astype(BF)
        store(t).start()
        return carry

    lax.fori_loop(0, tiles, project, 0)
    for t in range(tiles):
        store(t).wait()


def params(limit=66_000_000):
    return pltpu.CompilerParams(vmem_limit_bytes=limit)


def in_hbm(x):
    return pltpu.with_memory_space_constraint(x, pltpu.HBM)


def call_state(k, v, w, groups):
    chunks = 2
    any_block = pl.BlockSpec(memory_space=pl.ANY)
    shape = (groups, 5, 2, PAIR)
    return pl.pallas_call(
        state_kernel,
        in_specs=[any_block] * 3,
        out_specs=any_block,
        out_shape=jax.ShapeDtypeStruct(shape, BF),
        scratch_shapes=[pltpu.VMEM(k.shape, BF)] * 3
        + [
            pltpu.VMEM(shape, BF),
            pltpu.SemaphoreType.DMA((3, chunks)),
            pltpu.SemaphoreType.DMA((chunks,)),
        ],
        compiler_params=params(),
        cost_estimate=pl.CostEstimate(flops=4 << 30, bytes_accessed=4 << 20, transcendentals=1 << 20),
        name="state",
    )(k, v, w)


def call_local(side, r, k, v, w, g, bonus, gain):
    tokens, half = r.shape[0], gain.shape[1]
    chunks = 2
    any_block = pl.BlockSpec(memory_space=pl.ANY)
    vmem_block = pl.BlockSpec(memory_space=pltpu.VMEM)
    block = (tokens, half)
    return pl.pallas_call(
        local_kernel,
        in_specs=[pl.BlockSpec(memory_space=pltpu.SMEM)] + [vmem_block] * 2 + [any_block] * 5,
        out_specs=[vmem_block] * 3,
        out_shape=[jax.ShapeDtypeStruct(block, BF)] * 3,
        scratch_shapes=[pltpu.VMEM(block, BF)] * 5 + [pltpu.SemaphoreType.DMA((5, chunks))],
        compiler_params=params(limit=32 << 20),
        cost_estimate=pl.CostEstimate(flops=8 << 30, bytes_accessed=4 << 20, transcendentals=2 << 20),
        name="local",
    )(side, bonus, gain, r, k, v, w, g)


def call_scan(msg, anchor):
    shape = (msg.shape[0], 8, PAIR)
    return pl.pallas_call(
        scan_kernel,
        in_specs=[pl.BlockSpec(memory_space=pltpu.VMEM), pl.BlockSpec(memory_space=pl.ANY)],
        out_specs=pl.BlockSpec(memory_space=pl.ANY),
        out_shape=pltpu.HBM(shape, BF),
        scratch_shapes=[pltpu.VMEM(shape, BF), pltpu.SemaphoreType.DMA((4,))],
        compiler_params=params(limit=8 << 20),
        name="scan",
    )(msg, anchor)


def call_finish(core, entering, mine, other, weight, other_weight):
    half, cols = weight.shape
    tokens = mine[0].shape[0]
    tiles = 8
    any_block = pl.BlockSpec(memory_space=pl.ANY)
    return pl.pallas_call(
        finish_kernel,
        in_specs=[pl.BlockSpec(memory_space=pltpu.SMEM)]
        + [pl.BlockSpec(memory_space=pltpu.VMEM)] * 7
        + [any_block] * 2,
        out_specs=any_block,
        out_shape=jax.ShapeDtypeStruct((tokens, cols), BF),
        scratch_shapes=[
            pltpu.VMEM((2, half, cols), BF),
            pltpu.VMEM((2, tokens, half), F32),
            pltpu.VMEM((2, half // WIDE, WIDE, WIDE), BF),
            pltpu.VMEM((2, tokens, half), BF),
            pltpu.VMEM((tokens, cols), BF),
            pltpu.SemaphoreType.DMA((2, tiles)),
            pltpu.SemaphoreType.DMA((tiles,)),
        ],
        compiler_params=params(limit=32 << 20),
        name="finish",
    )(core, entering, *mine, *other, in_hbm(weight), in_hbm(other_weight))


def shards(r, k, v, w, g, bonus, gain, weight):
    groups = lax.axis_size(SEQ_HEAD)
    core = lax.axis_index("head").reshape(1).astype(jnp.int32)
    r, k, v, w, g = (in_hbm(x) for x in (r, k, v, w, g))
    gain = gain.reshape(1, -1)
    swap = [(0, 1), (1, 0)]
    other_weight = lax.ppermute(weight, "head", swap)
    msg = call_state(k, v, w, groups)
    msg = lax.all_to_all(msg, SEQ_HEAD, split_axis=0, concat_axis=0, tiled=True)
    mine = call_local(core, r, k, v, w, g, bonus, gain)
    entering = call_scan(msg, mine[1])
    entering = lax.all_to_all(entering, SEQ_HEAD, split_axis=0, concat_axis=0, tiled=True)
    _, bonus, gain = lax.optimization_barrier((mine[1], bonus, gain))
    bonus, gain = (lax.ppermute(x, "head", swap) for x in (bonus, gain))
    other = call_local(1 - core, r, k, v, w, g, bonus, gain)
    entering = entering.reshape(-1, HALF, PAIR)
    return call_finish(core, entering, mine, other, weight, other_weight)


def solution(mesh):
    torus = Mesh(mesh.devices.reshape(4, 4, 4, mesh.shape["head"]), SEQ_HEAD)
    in_specs = (P(SEQ_HEAD, None),) * 5 + (P("head", None), P("head"), P("head", None))
    return jax.shard_map(
        shards, mesh=torus, in_specs=in_specs, out_specs=P(SEQ_HEAD, None), check_vma=False
    )
```

```python
import jax
import jax.numpy as jnp
from jax import lax
from jax.experimental import pallas as pl
from jax.experimental.pallas import tpu as pltpu
from jax.sharding import Mesh
from jax.sharding import PartitionSpec as P


BLOCK = 128
HALF = 64
PAIR = 128
WIDE = 256
SEQ_HEAD = ("seq_0", "seq_1", "seq_2", "head")
EPS = 1e-05
LOG2E = 1.4426950408889634
LOG2LOG2E = 0.5287663729448977
TILES_AHEAD = 5
BF = jnp.bfloat16
F32 = jnp.float32


def mm(a, b):
    return lax.dot_general(a, b, (((1,), (0,)), ((), ())), preferred_element_type=F32)


def mm_nt(a, b):
    return lax.dot_general(a, b, (((1,), (1,)), ((), ())), preferred_element_type=F32)


def mm_tn(a, b):
    return lax.dot_general(a, b, (((0,), (0,)), ((), ())), preferred_element_type=F32)


def grid2(rows, cols):
    return (
        lax.broadcasted_iota(jnp.int32, (rows, cols), 0),
        lax.broadcasted_iota(jnp.int32, (rows, cols), 1),
    )


def two_parts(x):
    hi = x.astype(BF)
    return hi, (x - hi.astype(F32)).astype(BF)


def head_ones(scale):
    row, col = grid2(WIDE, WIDE)
    return jnp.where(row // HALF == col // HALF, scale, 0.0).astype(BF)


def decay_rate(w):
    return jnp.exp2(w.astype(F32) * LOG2E + LOG2LOG2E).astype(BF)


def centred(v):
    row, col = grid2(WIDE, WIDE)
    less_mean = jnp.where(row == col, 1.0, 0.0) - jnp.where(row // HALF == col // HALF, 1.0 / HALF, 0.0)
    return mm(v, less_mean.astype(BF)).astype(BF)


def state_kernel(k_hbm, v_hbm, w_hbm, msg_hbm, k_buf, v_buf, w_buf, msg_buf, in_sems, out_sems):
    tokens, width = k_buf.shape
    chunks = in_sems.shape[1]
    wide = width // chunks
    per = msg_buf.shape[0] // chunks
    loads = [
        [
            pltpu.make_async_copy(
                src.at[:, pl.ds(i * wide, wide)], dst.at[:, pl.ds(i * wide, wide)], in_sems.at[j, i]
            )
            for j, (src, dst) in enumerate(((w_hbm, w_buf), (k_hbm, k_buf), (v_hbm, v_buf)))
        ]
        for i in range(chunks)
    ]
    stores = [
        pltpu.make_async_copy(
            msg_buf.at[pl.ds(i * per, per)], msg_hbm.at[pl.ds(i * per, per)], out_sems.at[i]
        )
        for i in range(chunks)
    ]
    depth = chunks
    for chunk in loads[:depth]:
        for one in chunk:
            one.start()
    row, col = grid2(tokens, tokens)
    later = jnp.where(col > row, -1.0, 0.0).astype(BF)
    first = lax.broadcasted_iota(jnp.int32, (HALF, PAIR), 1) < HALF
    for i in range(chunks):
        for one in loads[i]:
            one.wait()
        for one in loads[i + depth] if i + depth < chunks else ():
            one.start()
        for part in range(i * wide // WIDE, (i + 1) * wide // WIDE):
            s = slice(part * WIDE, (part + 1) * WIDE)
            rate = decay_rate(w_buf[:, s])
            after = mm(later, rate)
            key_end = (k_buf[:, s].astype(F32) * jnp.exp2(after)).astype(BF)
            total = after[0:1] - rate[0:1].astype(F32)
            state = mm_tn(v_buf[:, s], key_end)
            tot_hi, tot_lo = two_parts(total)
            logs = jnp.concatenate([tot_hi, tot_lo], axis=0)
            for p in range(WIDE // PAIR):
                at = p * PAIR
                both = jnp.where(
                    first,
                    state[at : at + HALF, at : at + PAIR],
                    state[at + HALF : at + PAIR, at : at + PAIR],
                )
                both = (both - jnp.mean(both, axis=0, keepdims=True)).astype(BF)
                base = (part * (WIDE // PAIR) + p) * 8
                msg_buf[base : base + 8, 0:4] = both.reshape(8, 4, 2, PAIR)
                msg_buf[base : base + 8, 4] = jnp.broadcast_to(
                    logs[None, :, at : at + PAIR], (8, 2, PAIR)
                )
        stores[i].start()
    for one in stores:
        one.wait()


def local_kernel(
    h_ref,
    u_ref,
    gain_ref,
    r_hbm,
    k_hbm,
    v_hbm,
    w_hbm,
    g_hbm,
    out_ref,
    rin_ref,
    sg_ref,
    r_ref,
    k_ref,
    v_ref,
    w_ref,
    g_ref,
    in_sems,
):
    tokens, half = r_ref.shape
    chunks = in_sems.shape[1]
    wide = half // chunks
    sources = (w_hbm, g_hbm, r_hbm, k_hbm, v_hbm)
    buffers = (w_ref, g_ref, r_ref, k_ref, v_ref)

    def load(i):
        at = pl.ds(pl.multiple_of(h_ref[0] * half + i * wide, wide), wide)
        to = pl.ds(i * wide, wide)
        return [
            pltpu.make_async_copy(src.at[:, at], dst.at[:, to], in_sems.at[j, i])
            for j, (src, dst) in enumerate(zip(sources, buffers))
        ]

    for i in range(chunks):
        for one in load(i):
            one.start()
    row, col = grid2(tokens, tokens)
    upto = jnp.where(col <= row, -1.0, 0.0).astype(BF)
    prior = jnp.where(col < row, -1.0, 0.0).astype(BF)
    lane = lax.broadcasted_iota(jnp.int32, (BLOCK, PAIR), 1)
    first = lane < HALF
    zero = jnp.zeros((BLOCK, PAIR), BF)
    row, col = grid2(BLOCK, BLOCK)
    strict = row > col

    def stacked(x):
        return jnp.concatenate([jnp.where(first, x, zero), jnp.where(first, zero, x)], axis=0)

    def side(scores, masked):
        a, b = scores[:BLOCK], scores[BLOCK:]
        if masked:
            a, b = jnp.where(strict, a, 0.0), jnp.where(strict, b, 0.0)
        return jnp.concatenate([a, b], axis=1).astype(BF)

    def compute(part):
        at = part * WIDE
        c = slice(at, at + WIDE)
        gate = g_ref[:, c].astype(F32)
        sg_ref[:, c] = (0.5 * gate * (1.0 + jnp.tanh(0.5 * gate)) * gain_ref[:, c]).astype(BF)
        rate = decay_rate(w_ref[:, c])
        cum = mm(upto, rate)
        before = mm(prior, rate)
        r = r_ref[:, c]
        k = k_ref[:, c]
        v = centred(v_ref[:, c])
        mid0, end0, mid1 = cum[63:64], cum[127:128], cum[191:192]
        rf, kf = r.astype(F32), k.astype(F32)
        r0 = (rf[:BLOCK] * jnp.exp2(before[:BLOCK] - mid0)).astype(BF)
        k0 = (kf[:BLOCK] * jnp.exp2(mid0 - cum[:BLOCK])).astype(BF)
        r1 = (rf[BLOCK:] * jnp.exp2(before[BLOCK:] - mid1)).astype(BF)
        k1 = (kf[BLOCK:] * jnp.exp2(mid1 - cum[BLOCK:])).astype(BF)
        r1c = (rf[BLOCK:] * jnp.exp2(before[BLOCK:] - end0)).astype(BF)
        k0c = (kf[:BLOCK] * jnp.exp2(end0 - cum[:BLOCK])).astype(BF)
        rin_ref[:BLOCK, c] = (rf[:BLOCK] * jnp.exp2(before[:BLOCK])).astype(BF)
        rin_ref[BLOCK:, c] = (rf[BLOCK:] * jnp.exp2(before[BLOCK:])).astype(BF)
        heads = range(at // HALF, (at + WIDE) // HALF)
        u = jnp.concatenate([u_ref[h : h + 1] for h in heads], axis=1)
        bonus = (rf * u * kf).astype(BF)
        own = mm(bonus, head_ones(1.0)) * v.astype(F32)
        for p in range(WIDE // PAIR):
            s = slice(p * PAIR, (p + 1) * PAIR)
            o = slice(at + p * PAIR, at + (p + 1) * PAIR)
            s00 = side(mm_nt(stacked(r0[:, s]), k0[:, s]), True)
            s10 = side(mm_nt(stacked(r1c[:, s]), k0c[:, s]), False)
            s11 = side(mm_nt(stacked(r1[:, s]), k1[:, s]), True)
            v0, v1 = stacked(v[:BLOCK, s]), stacked(v[BLOCK:, s])
            out_ref[:BLOCK, o] = (mm(s00, v0) + own[:BLOCK, s]).astype(BF)
            out_ref[BLOCK:, o] = (mm(s10, v0) + mm(s11, v1) + own[BLOCK:, s]).astype(BF)

    for i in range(chunks):
        for one in load(i):
            one.wait()
        for part in range(i * wide // WIDE, (i + 1) * wide // WIDE):
            compute(part)


def scan_kernel(msg_ref, after_ref, out_hbm, out_ref, sems):
    groups = msg_ref.shape[0]
    pieces = sems.shape[0]
    per = groups // pieces
    stores = [
        pltpu.make_async_copy(out_ref.at[pl.ds(i * per, per)], out_hbm.at[pl.ds(i * per, per)], sems.at[i])
        for i in range(pieces)
    ]
    state = jnp.zeros((8, PAIR), F32)
    for g in range(groups):
        logs = msg_ref[g, 4].astype(F32)
        out_ref[g] = state.astype(BF)
        if g % per == per - 1:
            stores[g // per].start()
        decay = jnp.exp2(logs[0:1] + logs[1:2])
        state = state * decay + msg_ref[g, 0:4].reshape(8, PAIR).astype(F32)
    for one in stores:
        one.wait()


def finish_kernel(
    c_ref,
    s_ref,
    mine_out,
    mine_rin,
    mine_sg,
    other_out,
    other_rin,
    other_sg,
    w1_hbm,
    w2_hbm,
    y_hbm,
    w_buf,
    wkv_buf,
    entering,
    gated,
    y_buf,
    w_sems,
    y_sems,
):
    tiles = y_sems.shape[0] - 1
    half = mine_out.shape[1]
    tile = y_buf.shape[1] // tiles
    parts = half // WIDE
    results = ((mine_out, mine_rin, mine_sg), (other_out, other_rin, other_sg))

    def cols(t):
        return pl.ds(pl.multiple_of(t * tile, tile), tile)

    def fetch(j, t):
        src = (w1_hbm, w2_hbm)[j]
        return pltpu.make_async_copy(src.at[:, cols(t)], w_buf.at[j, :, cols(t)], w_sems.at[j, t])

    def store(t):
        return pltpu.make_async_copy(y_buf.at[:, cols(t)], y_hbm.at[:, cols(t)], y_sems.at[t])

    def end_cols(q):
        return pl.ds((tiles - 1) * tile + q * (tile // 2), tile // 2)

    def fetch_end(j, q):
        at, src = end_cols(q), (w1_hbm, w2_hbm)[j]
        sem = w_sems.at[j, tiles - 1 + q]
        return pltpu.make_async_copy(src.at[:, at], w_buf.at[j, :, at], sem)

    def store_end(q):
        at = end_cols(q)
        return pltpu.make_async_copy(y_buf.at[:, at], y_hbm.at[:, at], y_sems.at[tiles - 1 + q])

    for t in range(TILES_AHEAD):
        fetch(0, t).start()
        fetch(1, t).start()
    first = lax.broadcasted_iota(jnp.int32, (HALF, PAIR), 1) < HALF
    zero = jnp.zeros((HALF, PAIR), BF)
    share = head_ones(1.0 / HALF)
    for side in range(2):
        base = (c_ref[0] if side == 0 else 1 - c_ref[0]) * (half // PAIR)
        for part in range(parts):
            for p in range(2):
                pair = s_ref[base + 2 * part + p]
                lanes = slice(p * PAIR, (p + 1) * PAIR)
                rest = slice((1 - p) * PAIR, (2 - p) * PAIR)
                low, high = p * PAIR, p * PAIR + HALF
                entering[side, part, low:high, lanes] = jnp.where(first, pair, zero)
                entering[side, part, high : low + PAIR, lanes] = jnp.where(first, zero, pair)
                entering[side, part, low : low + PAIR, rest] = jnp.zeros((PAIR, PAIR), BF)
    for side in range(2):
        out_ref, rin_ref, _ = results[side]
        for part in range(parts):
            c = slice(part * WIDE, (part + 1) * WIDE)
            across = mm_nt(rin_ref[:, c], entering[side, part])
            wkv = out_ref[:, c].astype(F32) + across
            wkv_buf[side, :, c] = wkv
            gated[side, :, c] = (wkv * wkv).astype(BF)
    for side in range(2):
        sg_ref = results[side][2]
        for part in range(parts):
            c = slice(part * WIDE, (part + 1) * WIDE)
            var = mm(gated[side, :, c], share)
            gated[side, :, c] = (
                wkv_buf[side, :, c] * lax.rsqrt(var + EPS) * sg_ref[:, c].astype(F32)
            ).astype(BF)

    def project(t, carry):
        fetch(0, t).wait()
        fetch(1, t).wait()

        @pl.when(t + TILES_AHEAD < tiles - 1)
        def _():
            fetch(0, t + TILES_AHEAD).start()
            fetch(1, t + TILES_AHEAD).start()

        @pl.when(t + TILES_AHEAD == tiles - 1)
        def _():
            for q in range(2):
                for j in range(2):
                    fetch_end(j, q).start()

        y = mm(gated[0], w_buf[0, :, cols(t)]) + mm(gated[1], w_buf[1, :, cols(t)])
        y_buf[:, cols(t)] = y.astype(BF)
        store(t).start()
        return carry

    lax.fori_loop(0, tiles - 1, project, 0)
    for q in range(2):
        fetch_end(0, q).wait()
        fetch_end(1, q).wait()
        y = mm(gated[0], w_buf[0, :, end_cols(q)]) + mm(gated[1], w_buf[1, :, end_cols(q)])
        y_buf[:, end_cols(q)] = y.astype(BF)
        store_end(q).start()
    for t in range(tiles - 1):
        store(t).wait()
    for q in range(2):
        store_end(q).wait()


def params(limit=66_000_000):
    return pltpu.CompilerParams(vmem_limit_bytes=limit)


def in_hbm(x):
    return pltpu.with_memory_space_constraint(x, pltpu.HBM)


def call_state(k, v, w, groups):
    chunks = 2
    any_block = pl.BlockSpec(memory_space=pl.ANY)
    shape = (groups, 5, 2, PAIR)
    return pl.pallas_call(
        state_kernel,
        in_specs=[any_block] * 3,
        out_specs=any_block,
        out_shape=jax.ShapeDtypeStruct(shape, BF),
        scratch_shapes=[pltpu.VMEM(k.shape, BF)] * 3
        + [
            pltpu.VMEM(shape, BF),
            pltpu.SemaphoreType.DMA((3, chunks)),
            pltpu.SemaphoreType.DMA((chunks,)),
        ],
        compiler_params=params(),
        cost_estimate=pl.CostEstimate(flops=4 << 30, bytes_accessed=4 << 20, transcendentals=1 << 20),
        name="state",
    )(k, v, w)


def call_local(side, r, k, v, w, g, bonus, gain):
    tokens, half = r.shape[0], gain.shape[1]
    chunks = 2
    any_block = pl.BlockSpec(memory_space=pl.ANY)
    vmem_block = pl.BlockSpec(memory_space=pltpu.VMEM)
    block = (tokens, half)
    return pl.pallas_call(
        local_kernel,
        in_specs=[pl.BlockSpec(memory_space=pltpu.SMEM)] + [vmem_block] * 2 + [any_block] * 5,
        out_specs=[vmem_block] * 3,
        out_shape=[jax.ShapeDtypeStruct(block, BF)] * 3,
        scratch_shapes=[pltpu.VMEM(block, BF)] * 5 + [pltpu.SemaphoreType.DMA((5, chunks))],
        compiler_params=params(limit=32 << 20),
        cost_estimate=pl.CostEstimate(flops=8 << 30, bytes_accessed=4 << 20, transcendentals=2 << 20),
        name="local",
    )(side, bonus, gain, r, k, v, w, g)


def call_scan(msg, anchor):
    shape = (msg.shape[0], 8, PAIR)
    return pl.pallas_call(
        scan_kernel,
        in_specs=[pl.BlockSpec(memory_space=pltpu.VMEM), pl.BlockSpec(memory_space=pl.ANY)],
        out_specs=pl.BlockSpec(memory_space=pl.ANY),
        out_shape=pltpu.HBM(shape, BF),
        scratch_shapes=[pltpu.VMEM(shape, BF), pltpu.SemaphoreType.DMA((4,))],
        compiler_params=params(limit=8 << 20),
        name="scan",
    )(msg, anchor)


def call_finish(core, entering, mine, other, weight, other_weight):
    half, cols = weight.shape
    tokens = mine[0].shape[0]
    tiles = 8
    any_block = pl.BlockSpec(memory_space=pl.ANY)
    return pl.pallas_call(
        finish_kernel,
        in_specs=[pl.BlockSpec(memory_space=pltpu.SMEM)]
        + [pl.BlockSpec(memory_space=pltpu.VMEM)] * 7
        + [any_block] * 2,
        out_specs=any_block,
        out_shape=jax.ShapeDtypeStruct((tokens, cols), BF),
        scratch_shapes=[
            pltpu.VMEM((2, half, cols), BF),
            pltpu.VMEM((2, tokens, half), F32),
            pltpu.VMEM((2, half // WIDE, WIDE, WIDE), BF),
            pltpu.VMEM((2, tokens, half), BF),
            pltpu.VMEM((tokens, cols), BF),
            pltpu.SemaphoreType.DMA((2, tiles + 1)),
            pltpu.SemaphoreType.DMA((tiles + 1,)),
        ],
        compiler_params=params(limit=32 << 20),
        name="finish",
    )(core, entering, *mine, *other, in_hbm(weight), in_hbm(other_weight))


def shards(r, k, v, w, g, bonus, gain, weight):
    groups = lax.axis_size(SEQ_HEAD)
    core = lax.axis_index("head").reshape(1).astype(jnp.int32)
    r, k, v, w, g = (in_hbm(x) for x in (r, k, v, w, g))
    gain = gain.reshape(1, -1)
    swap = [(0, 1), (1, 0)]
    other_weight = lax.ppermute(weight, "head", swap)
    msg = call_state(k, v, w, groups)
    msg = lax.all_to_all(msg, SEQ_HEAD, split_axis=0, concat_axis=0, tiled=True)
    mine = call_local(core, r, k, v, w, g, bonus, gain)
    entering = call_scan(msg, mine[1])
    entering = lax.all_to_all(entering, SEQ_HEAD, split_axis=0, concat_axis=0, tiled=True)
    _, bonus, gain = lax.optimization_barrier((mine[1], bonus, gain))
    bonus, gain = (lax.ppermute(x, "head", swap) for x in (bonus, gain))
    other = call_local(1 - core, r, k, v, w, g, bonus, gain)
    entering = entering.reshape(-1, HALF, PAIR)
    return call_finish(core, entering, mine, other, weight, other_weight)


def solution(mesh):
    torus = Mesh(mesh.devices.reshape(4, 4, 4, mesh.shape["head"]), SEQ_HEAD)
    in_specs = (P(SEQ_HEAD, None),) * 5 + (P("head", None), P("head"), P("head", None))
    return jax.shard_map(
        shards, mesh=torus, in_specs=in_specs, out_specs=P(SEQ_HEAD, None), check_vma=False
    )
```
